32 devices in a mesh: box: 4 (over z), tile: 8 (over y, x, core).
Axes of the slice: x: 2, y: 2, z: 4, core: 2. Of those that a mesh axis runs over, the one named last changes fastest.
Arguments:
- box_maps: float32 [4, 6, 448, 2688], P('box', None, 'tile'), may hold values from -4.01 to 4.01, as said below
- face_slots: int32 [4, 6], replicated, may hold values from 0 to 5, each once within a row
Outputs:
- final_map: float32 [7168, 7168], P('tile', 'box')
The draws below stay inside these ranges and needn't reach their ends.
Inputs may be any that keep to these rules, and one draw needn't show every extreme that they name: `box_maps`: read as a matrix of order 6 * 448 with rows and columns ordered by stored block and node, each box's map is exactly symmetric and positive definite. `face_slots`: each row is a permutation of the six stored blocks.
All inputs are finite; a program needn't handle non-finite values.
Results may differ from the reference program's by a relative error of at most 0.0001.
Values sent between devices are 32-bit elements; how exact they have to be, the bound alone decides.
A program may use at most 128 MiB of HBM per device.

```python
import math
import jax
import jax.numpy as jnp
from jax import lax

F = 448


def draw_box_maps(key, part):
    extent = 6 * F
    factor_key, weight_key = jax.random.split(jax.random.fold_in(key, 11), 2)
    factors = jax.random.truncated_normal(factor_key, -3.0, 3.0, (4, extent, extent), jnp.float32)
    weights = jnp.exp(jax.random.uniform(weight_key, (4, 1, extent), jnp.float32, math.log(0.05), math.log(5.0)))
    gramian = jnp.einsum('bik,bjk->bij', factors * weights, factors, precision=lax.Precision.HIGHEST) / extent
    matrices = gramian + 0.1 * jnp.eye(extent, dtype=jnp.float32)
    largest = jnp.max(jnp.diagonal(matrices, 0, 1, 2), axis=1)
    matrices = matrices * (4.0 / largest)[:, None, None]
    matrices = (matrices + jnp.swapaxes(matrices, 1, 2)) * 0.5
    return matrices.reshape(4, 6, F, extent)


def setup_inputs(seed: int = 0) -> dict:
    keys = jax.random.split(jax.random.key(seed), 3)
    return {
        "box_maps": draw_box_maps(jax.random.fold_in(keys[2], 71), 0),
        "face_slots": jax.vmap(lambda own: jax.random.permutation(own, 6))(jax.random.split(keys[1], 4)).reshape((4, 6)).astype(jnp.int32),
    }


def matmul(left, right):
    return jnp.dot(left.astype(jnp.float32), right.astype(jnp.float32), precision=lax.Precision.HIGHEST, preferred_element_type=jnp.float32)

def lower_solve(factor, coupled):
    return jax.scipy.linalg.solve_triangular(factor, coupled.T, lower=True).T

def reference(box_maps, face_slots):
    matrices = box_maps.reshape(4, 6 * F, 6 * F)

    def face_block(box_id, row_face, col_face):
        row_start = (face_slots[box_id, row_face] * F).astype(jnp.int32)
        col_start = (face_slots[box_id, col_face] * F).astype(jnp.int32)
        return lax.dynamic_slice(matrices[box_id], (row_start, col_start), (F, F))
    layouts = []
    for box_id in range(4):
        along_x, along_y = (box_id % 2, box_id // 2)
        layouts.append((1 - along_x, [along_x, 2 + along_y, 4, 5], 3 - along_y))
    level_one = []
    for pair_id in range(2):
        left_box, right_box = (2 * pair_id, 2 * pair_id + 1)
        summed = face_block(left_box, layouts[left_box][0], layouts[left_box][0]) + face_block(right_box, layouts[right_box][0], layouts[right_box][0])
        factor = jnp.linalg.cholesky(summed)
        for box_id in (left_box, right_box):
            x_shared, finals, y_shared = layouts[box_id]
            coupled = jnp.concatenate([face_block(box_id, surface, x_shared) for surface in finals + [y_shared]], 0)
            level_one.append(lower_solve(factor, coupled))
    zero_block = jnp.zeros((F, F), jnp.float32)
    pair_terms = []
    shared_rows = []
    for pair_id in range(2):
        left_box, right_box = (2 * pair_id, 2 * pair_id + 1)
        stacked = jnp.concatenate([level_one[left_box][4 * F:], level_one[right_box][4 * F:]], 0)
        shared_rows.append(stacked)
        left_face = face_block(left_box, layouts[left_box][2], layouts[left_box][2])
        right_face = face_block(right_box, layouts[right_box][2], layouts[right_box][2])
        diagonal = jnp.concatenate([jnp.concatenate([left_face, zero_block], 1), jnp.concatenate([zero_block, right_face], 1)], 0)
        pair_terms.append(diagonal - matmul(stacked, stacked.T))
    factor_two = jnp.linalg.cholesky(pair_terms[0] + pair_terms[1])
    level_two = []
    for box_id in range(4):
        x_shared, finals, y_shared = layouts[box_id]
        direct = jnp.concatenate([face_block(box_id, surface, y_shared) for surface in finals], 0)
        empty_part = jnp.zeros_like(direct)
        placed = jnp.concatenate([direct, empty_part] if box_id % 2 == 0 else [empty_part, direct], 1)
        coupled = placed - matmul(level_one[box_id][:4 * F], shared_rows[box_id // 2].T)
        level_two.append(lower_solve(factor_two, coupled))
    row_blocks = []
    for box_id in range(4):
        finals = layouts[box_id][1]
        entries = []
        for column_box in range(4):
            entry_block = jnp.zeros((4 * F, 4 * F), jnp.float32)
            if column_box == box_id:
                entry_block = entry_block + jnp.concatenate([jnp.concatenate([face_block(box_id, surface, other_face) for other_face in finals], 1) for surface in finals], 0)
            if column_box // 2 == box_id // 2:
                entry_block = entry_block - matmul(level_one[box_id][:4 * F], level_one[column_box][:4 * F].T)
            entry_block = entry_block - matmul(level_two[box_id], level_two[column_box].T)
            entries.append(entry_block)
        row_blocks.append(jnp.concatenate(entries, 1))
    return jnp.concatenate(row_blocks, 0)
```

```python
import jax
import jax.numpy as jnp
from jax import lax
from jax.experimental import pallas as pl
from jax.experimental.pallas import tpu as pltpu
from jax.sharding import PartitionSpec as P

MESH = pl.DeviceIdType.MESH
HIGHEST = lax.Precision.HIGHEST
HIGH = lax.Precision.HIGH
BLOCK = 64
LANES = 128


def dot(left, right, precision=HIGHEST):
    return jnp.dot(left, right, precision=precision, preferred_element_type=jnp.float32)


def dot_nt(left, right, precision=HIGHEST):
    return lax.dot_general(
        left, right, (((1,), (1,)), ((), ())), precision=precision, preferred_element_type=jnp.float32
    )


def face_order(box_id):
    along_x, along_y = box_id % 2, box_id // 2
    return 1 - along_x, (along_x, 2 + along_y, 4, 5), 3 - along_y


def pick_kernel(slots_ref, stored_ref, shared_ref, rows_ref, own_ref):
    size = shared_ref.shape[-1]
    box_id = lax.axis_index("box")
    x_face, final_faces, y_face = face_order(box_id)
    slot_of = [slots_ref[box_id, face] for face in (x_face, y_face) + final_faces]
    width = -(-(size + BLOCK) // LANES) * LANES

    def piece(row_slot, col_slot):
        start = col_slot * size
        low = start // LANES * LANES
        window = stored_ref[row_slot, :, pl.ds(pl.multiple_of(low, LANES), width)]
        return jnp.where(start == low, window[:, :size], window[:, BLOCK : BLOCK + size])

    x_slot, y_slot, *finals = slot_of
    shared_ref[0] = piece(x_slot, x_slot)
    shared_ref[1] = piece(y_slot, x_slot)
    shared_ref[2] = piece(y_slot, y_slot)
    for index, row_slot in enumerate(finals):
        rows_ref[index] = jnp.concatenate([piece(row_slot, x_slot), piece(row_slot, y_slot)], 1)
        own_ref[index] = jnp.concatenate([piece(row_slot, col_slot) for col_slot in finals], 1)


def pick_faces(stored, face_slots):
    _, nodes, extent = stored.shape
    size = extent // 6
    return pl.pallas_call(
        pick_kernel,
        out_shape=[
            jax.ShapeDtypeStruct((3, nodes, size), jnp.float32),
            jax.ShapeDtypeStruct((4, nodes, 2 * size), jnp.float32),
            jax.ShapeDtypeStruct((4, nodes, 4 * size), jnp.float32),
        ],
        in_specs=[pl.BlockSpec(memory_space=pltpu.SMEM), pl.BlockSpec(memory_space=pltpu.VMEM)],
        out_specs=[pl.BlockSpec(memory_space=pltpu.VMEM)] * 3,
        name="pick_faces",
    )(face_slots, stored)


def leaf_inverse(work_ref):
    size = work_ref.shape[0]

    def octet(index, carry):
        base = pl.multiple_of(index * 8, 8)
        whole = work_ref[...]
        panel = work_ref[pl.ds(base, 8), :]
        lanes = lax.broadcasted_iota(jnp.int32, whole.shape, 1)
        rows = lax.broadcasted_iota(jnp.int32, whole.shape, 0)
        panel_lanes = lax.broadcasted_iota(jnp.int32, panel.shape, 1)
        panel_rows = lax.broadcasted_iota(jnp.int32, panel.shape, 0)
        cols = [
            jnp.broadcast_to(jnp.sum(jnp.where(lanes == base + j, whole, 0.0), 1, keepdims=True), whole.shape)
            for j in range(8)
        ]
        pivots = [
            jnp.broadcast_to(
                jnp.sum(jnp.where(panel_lanes == base + j, panel, 0.0), 1, keepdims=True), panel.shape
            )
            for j in range(8)
        ]
        change = jnp.zeros_like(whole)
        for j in range(8):
            inverse = 1.0 / pivots[j][j : j + 1]
            others = jnp.where(panel_rows != j, pivots[j] * inverse, 0.0)
            scaled = cols[j] * inverse
            for k in range(j + 1, 8):
                head = pivots[k][j : j + 1]
                pivots[k] = pivots[k] - others * head
                cols[k] = cols[k] - scaled * head
            row = panel[j : j + 1]
            change = change + scaled * row
            panel = panel - others * row
        inside = jnp.logical_and(rows >= base, rows < base + 8)
        work_ref[...] = jnp.where(inside, whole, whole - change)
        work_ref[pl.ds(base, 8), :] = panel
        return carry

    lax.fori_loop(0, size // 8, octet, 0)
    done = work_ref[...]
    lanes = lax.broadcasted_iota(jnp.int32, done.shape, 1)
    rows = lax.broadcasted_iota(jnp.int32, done.shape, 0)
    diagonal = jnp.sum(jnp.where(lanes == rows, done, 0.0), 1, keepdims=True)
    return done[:, size:] * (1.0 / diagonal)


def invert(ref, work_ref, between):
    order = ref.shape[0]
    row_ids = lax.broadcasted_iota(jnp.int32, (BLOCK, BLOCK), 0)
    col_ids = lax.broadcasted_iota(jnp.int32, (BLOCK, BLOCK), 1)
    eye = jnp.where(row_ids == col_ids, 1.0, 0.0).astype(jnp.float32)
    for start in range(0, order, BLOCK):
        stop = start + BLOCK
        work_ref[...] = jnp.concatenate([ref[start:stop, start:stop], eye], 1)
        inverse = leaf_inverse(work_ref)
        left = ref[:, start:stop]
        ids = lax.broadcasted_iota(jnp.int32, left.shape, 0)
        left = jnp.where(jnp.logical_and(ids >= start, ids < stop), 0.0, left)
        ref[:, start:stop] = jnp.zeros((order, BLOCK), jnp.float32)
        ref[start:stop, start:stop] = eye
        panel = dot(inverse, ref[start:stop, :])
        ref[start:stop, :] = panel
        ref[...] -= dot(left, panel)
        between()


def merge_kernel(
    tiles,
    shared_ref,
    rows_ref,
    own_ref,
    middle_ref,
    wide_ref,
    tall_ref,
    exact_ref,
    z_ref,
    sum_ref,
    part_ref,
    far_ref,
    inv_ref,
    couple_ref,
    half_ref,
    other_ref,
    full_ref,
    link_ref,
    temp_ref,
    work_ref,
    z_sems,
    part_sems,
    far_sems,
    wide_sems,
    twin_sems,
    tall_sems,
    exact_sems,
    swap_sems,
    local_sems,
):
    size = shared_ref.shape[-1]
    nodes = shared_ref.shape[1]
    boxes = z_ref.shape[1]
    slots = tall_ref.shape[0]
    box_id = lax.axis_index("box")
    tile_id = lax.axis_index("tile")
    core = tile_id % 2
    twin = tile_id + 1 - 2 * core

    def remote(source, target, sems, index, box, tile):
        return pltpu.make_async_remote_copy(
            src_ref=source,
            dst_ref=target,
            send_sem=sems.at[(0,) + index],
            recv_sem=sems.at[(1,) + index],
            device_id={"box": box, "tile": tile},
            device_id_type=MESH,
        )

    def each(low, high, action):
        def step(index, carry):
            action(index)
            return carry

        lax.fori_loop(low, high, step, 0)

    barrier = pltpu.get_barrier_semaphore()

    def greet(box, tile):
        pl.semaphore_signal(barrier, inc=1, device_id={"box": box, "tile": tile}, device_id_type=MESH)

    each(1, boxes, lambda i: greet((box_id + i) % boxes, tile_id))
    each(1, tiles, lambda i: greet(box_id, (tile_id + i) % tiles))
    pl.semaphore_wait(barrier, boxes + tiles - 2)

    def z_copy(kind, i, sender):
        return remote(
            shared_ref.at[kind], z_ref.at[kind, sender], z_sems, (kind, i - 1), (box_id + i) % boxes, tile_id
        )

    for kind in range(3):
        each(1, boxes, lambda i: z_copy(kind, i, box_id).start())
        z_ref[kind, box_id] = shared_ref[kind]

    def part_copy(kind, i, sender):
        tile = (tile_id + i) % tiles
        pair = tile % 2
        if kind == 1:
            source, target = z_ref.at[1, pl.ds(2 * pair, 2)], part_ref.at[pl.ds(1, 2), sender]
        else:
            source, target = sum_ref.at[pair, kind // 2], part_ref.at[kind // 2 * 3, sender]
        return remote(source, target, part_sems, (kind, i - 1), box_id, tile)

    def z_wait(kind):
        each(1, boxes, lambda i: z_copy(kind, i, (box_id + boxes - i) % boxes).wait_recv())

    z_wait(0)
    for pair in range(2):
        sum_ref[pair, 0] = z_ref[0, 2 * pair] + z_ref[0, 2 * pair + 1]
    each(1, tiles, lambda i: part_copy(0, i, tile_id).start())
    z_wait(1)
    each(1, tiles, lambda i: part_copy(1, i, tile_id).start())
    z_wait(2)
    for pair in range(2):
        sum_ref[pair, 1] = z_ref[2, pair] + z_ref[2, pair + 2]
    each(1, tiles, lambda i: part_copy(2, i, tile_id).start())
    part_ref[0, tile_id] = sum_ref[core, 0]
    part_ref[1, tile_id] = z_ref[1, 2 * core]
    part_ref[2, tile_id] = z_ref[1, 2 * core + 1]
    part_ref[3, tile_id] = sum_ref[core, 1]

    def far_copy(i, sender):
        return remote(rows_ref, far_ref.at[sender], far_sems, (i - 1,), (box_id + i) % boxes, tile_id)

    each(1, boxes, lambda i: far_copy(i, box_id).start())

    def wide_copy(i, sender):
        return remote(
            rows_ref, wide_ref.at[:, sender], wide_sems, (i - 1,), box_id, (tile_id + 2 * i) % tiles
        )

    def twin_copy(i, sender):
        source = rows_ref if i is None else wide_ref.at[:, sender]
        index = (0,) if i is None else (i,)
        return remote(source, wide_ref.at[:, sender], twin_sems, index, box_id, twin)

    each(1, tiles // 2, lambda i: wide_copy(i, tile_id).start())
    twin_copy(None, tile_id).start()
    keep = pltpu.make_async_copy(rows_ref, wide_ref.at[:, tile_id], local_sems.at[0])
    keep.start()

    def owner(box, face, tile):
        flat = (box * 4 + face) * tiles + tile
        return flat // slots, flat % slots

    def placed(box, face, remote_action, local_action, source, target_ref, sems, local_index):
        dest, slot = owner(box, face, tile_id)

        @pl.when(dest == tile_id)
        def _():
            local_action(pltpu.make_async_copy(source, target_ref.at[slot], local_sems.at[local_index]))

        @pl.when(dest != tile_id)
        def _():
            remote_action(
                pltpu.make_async_remote_copy(
                    src_ref=source,
                    dst_ref=target_ref.at[slot],
                    send_sem=sems.at[0, local_index - 1],
                    recv_sem=sems.at[1, slot],
                    device_id={"box": box_id, "tile": dest},
                    device_id_type=MESH,
                )
            )

    def exact_move(face, remote_action, local_action):
        placed(box_id, face, remote_action, local_action, own_ref.at[face], exact_ref, exact_sems, 1 + face)

    def tall_move(i, face, remote_action, local_action):
        box = (box_id + boxes - i) % boxes
        index = 1 + 4 * i + face
        placed(box, face, remote_action, local_action, far_ref.at[box, face], tall_ref, tall_sems, index)

    def start(copy):
        copy.start()

    for face in range(4):
        exact_move(face, start, start)

    def forward_wide(i):
        sender = (tile_id + tiles - 2 * i) % tiles
        wide_copy(i, sender).wait_recv()
        twin_copy(i, sender).start()

    def forward_tall(i):
        far_copy(i, (box_id + boxes - i) % boxes).wait_recv()
        for face in range(4):
            tall_move(i, face, start, start)

    pending = []

    def between():
        if pending:
            action = pending.pop(0)
            if action is not None:
                action()

    def part_wait(kind):
        each(1, tiles, lambda i: part_copy(kind, i, (tile_id + tiles - i) % tiles).wait_recv())

    def matrix(kind):
        if nodes % 8 == 0:
            return part_ref[kind].reshape(tiles * nodes, size)
        for tile in range(tiles):
            temp_ref[tile * nodes : (tile + 1) * nodes, :] = part_ref[kind, tile]
        return temp_ref[...]

    def swap(ref, index):
        return remote(ref, ref, swap_sems, (index,), box_id, twin)

    part_wait(0)
    inv_ref[core] = matrix(0)
    invert(inv_ref.at[core], work_ref, between)
    swap(inv_ref.at[core], 0).start()
    part_wait(1)
    for side in range(2):
        link_ref[side] = matrix(1 + side)
        couple_ref[core, side] = dot(link_ref[side], inv_ref[core])
    swap(couple_ref.at[core], 1).start()
    part_wait(2)
    shared = matrix(3)
    half_ref[0] = jnp.where(core == 0, shared, 0.0) - dot_nt(couple_ref[core, 0], link_ref[0])
    half_ref[1] = -dot_nt(couple_ref[core, 0], link_ref[1])
    half_ref[2] = jnp.where(core == 1, shared, 0.0) - dot_nt(couple_ref[core, 1], link_ref[1])

    def half_swap(index):
        return remote(half_ref.at[index], other_ref.at[index], swap_sems, (2 + index,), box_id, twin)

    for index in range(3):
        half_swap(index).start()
    pending.extend([None, lambda: forward_tall(1), None, lambda: forward_tall(3), None])
    pending.extend([lambda: each(1, tiles // 2, forward_wide), None, None, lambda: forward_tall(2)])
    half_swap(0).wait_recv()
    full_ref[0, 0] = half_ref[0] + other_ref[0]
    invert(full_ref.at[0, 0], work_ref, between)
    half_swap(1).wait_recv()
    half_swap(2).wait_recv()
    cross = half_ref[1] + other_ref[1]
    temp_ref[...] = dot(full_ref[0, 0], cross)
    full_ref[1, 1] = half_ref[2] + other_ref[2] - dot(cross.T, temp_ref[...])
    invert(full_ref.at[1, 1], work_ref, between)
    while pending:
        between()
    full_ref[0, 1] = -dot(temp_ref[...], full_ref[1, 1])
    full_ref[1, 0] = full_ref[0, 1].T
    full_ref[0, 0] = full_ref[0, 0] - dot_nt(full_ref[0, 1], temp_ref[...])

    def swap_in(ref, index):
        return remote(ref, ref, swap_sems, (index,), box_id, twin)

    swap_in(inv_ref.at[1 - core], 0).wait_recv()
    swap_in(couple_ref.at[1 - core], 1).wait_recv()
    row_box = tile_id * boxes // tiles
    row_pair, row_side = row_box // 2, row_box % 2
    col_pair, col_side = box_id // 2, box_id % 2
    for side in range(2):
        link_ref[side] = dot(full_ref[side, 0], couple_ref[col_pair, 0], HIGH) + dot(
            full_ref[side, 1], couple_ref[col_pair, 1], HIGH
        )
    temp_ref[...] = dot(full_ref[col_side, 0], couple_ref[row_pair, 0], HIGH) + dot(
        full_ref[col_side, 1], couple_ref[row_pair, 1], HIGH
    )
    middle_ref[:size, size:] = -temp_ref[...].T
    middle_ref[size:, :size] = -link_ref[row_side]
    middle_ref[size:, size:] = full_ref[row_side, col_side]
    corner = dot(couple_ref[row_pair, 0].T, link_ref[0], HIGH) + dot(
        couple_ref[row_pair, 1].T, link_ref[1], HIGH
    )
    middle_ref[:size, :size] = corner + jnp.where(row_pair == col_pair, inv_ref[row_pair], 0.0)

    def twin_wait(i):
        sender = (twin + tiles - 2 * i) % tiles
        twin_copy(i, sender).wait_recv()

    each(0, tiles // 2, twin_wait)

    def slot_wait(slot):
        source = (tile_id * slots + slot) % tiles

        @pl.when(jnp.logical_and(source != tile_id, row_box != box_id))
        def _():
            remote(rows_ref.at[0], tall_ref.at[slot], tall_sems, (slot,), box_id, twin).wait_recv()

        @pl.when(jnp.logical_and(source != tile_id, row_box == box_id))
        def _():
            remote(own_ref.at[0], exact_ref.at[slot], exact_sems, (slot,), box_id, twin).wait_recv()

    each(0, slots, slot_wait)

    def sent(copy):
        copy.wait_send()

    def done(copy):
        copy.wait()

    for face in range(4):
        exact_move(face, sent, done)
        for i in range(1, boxes):
            tall_move(i, face, sent, done)
    keep.wait()
    for kind in range(3):
        each(1, boxes, lambda i: z_copy(kind, i, box_id).wait_send())
        each(1, tiles, lambda i: part_copy(kind, i, tile_id).wait_send())
    each(1, boxes, lambda i: far_copy(i, box_id).wait_send())
    each(1, tiles // 2, lambda i: wide_copy(i, tile_id).wait_send())
    twin_copy(None, tile_id).wait_send()
    each(1, tiles // 2, lambda i: twin_copy(i, (tile_id + tiles - 2 * i) % tiles).wait_send())
    swap(inv_ref.at[core], 0).wait_send()
    swap(couple_ref.at[core], 1).wait_send()
    for index in range(3):
        half_swap(index).wait_send()


def merge(shared, rows, own):
    _, nodes, size = shared.shape
    tiles, boxes = lax.axis_size("tile"), lax.axis_size("box")
    slots = 4 * boxes
    square = (size, size)

    def vmem(*shape):
        return pltpu.VMEM(shape, jnp.float32)

    def sems(*shape):
        return pltpu.SemaphoreType.DMA((2,) + shape)

    def kernel(*refs):
        merge_kernel(tiles, *refs)

    return pl.pallas_call(
        kernel,
        out_shape=[
            jax.ShapeDtypeStruct((2 * size, 2 * size), jnp.float32),
            jax.ShapeDtypeStruct((4, tiles, nodes, 2 * size), jnp.float32),
            jax.ShapeDtypeStruct((slots, nodes, 2 * size), jnp.float32),
            jax.ShapeDtypeStruct((slots, nodes, 4 * size), jnp.float32),
        ],
        in_specs=[pl.BlockSpec(memory_space=pltpu.VMEM)] * 3,
        out_specs=[pl.BlockSpec(memory_space=pltpu.VMEM)] + [pl.BlockSpec(memory_space=pltpu.HBM)] * 3,
        scratch_shapes=[
            vmem(3, boxes, nodes, size),
            vmem(2, 2, nodes, size),
            vmem(4, tiles, nodes, size),
            vmem(boxes, 4, nodes, 2 * size),
            vmem(2, *square),
            vmem(2, 2, *square),
            vmem(3, *square),
            vmem(3, *square),
            vmem(2, 2, *square),
            vmem(2, *square),
            vmem(*square),
            vmem(BLOCK, 2 * BLOCK),
            sems(3, boxes - 1),
            sems(3, tiles - 1),
            sems(boxes - 1),
            sems(tiles // 2),
            sems(tiles // 2),
            sems(slots),
            sems(slots),
            sems(5),
            pltpu.SemaphoreType.DMA((1 + 4 * boxes,)),
        ],
        compiler_params=pltpu.CompilerParams(
            collective_id=0, has_side_effects=True, vmem_limit_bytes=60 * 2**20
        ),
        name="merge",
    )(shared, rows, own)


def per_device(box_maps, face_slots):
    shared, rows, own = pick_faces(box_maps[0], face_slots)
    _, nodes, size = shared.shape
    middle, wide, tall, exact = merge(shared, rows, own)
    tiles, boxes = lax.axis_size("tile"), lax.axis_size("box")
    box_id, tile_id = lax.axis_index("box"), lax.axis_index("tile")
    count = tall.shape[0] * nodes
    wide = wide.reshape(4 * tiles * nodes, 2 * size)
    same = tile_id * boxes // tiles == box_id
    offset = (tile_id % (tiles // boxes)) * count
    tall = jnp.where(
        same, lax.dynamic_slice_in_dim(wide, offset, count, 0), tall.reshape(count, 2 * size)
    )
    left = dot(tall, middle, HIGH)
    return jnp.where(same, exact.reshape(count, 4 * size), 0.0) - dot_nt(left, wide, HIGH)


def solution(mesh):
    return jax.shard_map(
        per_device,
        mesh=mesh,
        in_specs=(P("box", None, "tile", None), P()),
        out_specs=P("tile", "box"),
        check_vma=False,
    )
```

```python
import jax
import jax.numpy as jnp
from jax import lax
from jax.experimental import pallas as pl
from jax.experimental.pallas import tpu as pltpu
from jax.sharding import PartitionSpec as P

MESH = pl.DeviceIdType.MESH
HIGHEST = lax.Precision.HIGHEST
HIGH = lax.Precision.HIGH
BLOCK = 64
LANES = 128


def dot(left, right, precision=HIGHEST):
    return jnp.dot(left, right, precision=precision, preferred_element_type=jnp.float32)


def dot_nt(left, right, precision=HIGHEST):
    return lax.dot_general(
        left, right, (((1,), (1,)), ((), ())), precision=precision, preferred_element_type=jnp.float32
    )


def face_order(box_id):
    along_x, along_y = box_id % 2, box_id // 2
    return 1 - along_x, (along_x, 2 + along_y, 4, 5), 3 - along_y


def pick_kernel(slots_ref, stored_ref, shared_ref, rows_ref, own_ref):
    size = shared_ref.shape[-1]
    box_id = lax.axis_index("box")
    x_face, final_faces, y_face = face_order(box_id)
    slot_of = [slots_ref[box_id, face] for face in (x_face, y_face) + final_faces]
    width = -(-(size + BLOCK) // LANES) * LANES

    def piece(row_slot, col_slot):
        start = col_slot * size
        low = start // LANES * LANES
        window = stored_ref[row_slot, :, pl.ds(pl.multiple_of(low, LANES), width)]
        return jnp.where(start == low, window[:, :size], window[:, BLOCK : BLOCK + size])

    x_slot, y_slot, *finals = slot_of
    shared_ref[0] = piece(x_slot, x_slot)
    shared_ref[1] = piece(y_slot, x_slot)
    shared_ref[2] = piece(y_slot, y_slot)
    for index, row_slot in enumerate(finals):
        rows_ref[index] = jnp.concatenate([piece(row_slot, x_slot), piece(row_slot, y_slot)], 1)
        own_ref[index] = jnp.concatenate([piece(row_slot, col_slot) for col_slot in finals], 1)


def pick_faces(stored, face_slots):
    _, nodes, extent = stored.shape
    size = extent // 6
    return pl.pallas_call(
        pick_kernel,
        out_shape=[
            jax.ShapeDtypeStruct((3, nodes, size), jnp.float32),
            jax.ShapeDtypeStruct((4, nodes, 2 * size), jnp.float32),
            jax.ShapeDtypeStruct((4, nodes, 4 * size), jnp.float32),
        ],
        in_specs=[pl.BlockSpec(memory_space=pltpu.SMEM), pl.BlockSpec(memory_space=pltpu.VMEM)],
        out_specs=[pl.BlockSpec(memory_space=pltpu.VMEM)] * 3,
        name="pick_faces",
    )(face_slots, stored)


def leaf_inverse(work_ref):
    size = work_ref.shape[0]

    def octet(index, carry):
        base = pl.multiple_of(index * 8, 8)
        whole = work_ref[...]
        panel = work_ref[pl.ds(base, 8), :]
        lanes = lax.broadcasted_iota(jnp.int32, whole.shape, 1)
        rows = lax.broadcasted_iota(jnp.int32, whole.shape, 0)
        panel_lanes = lax.broadcasted_iota(jnp.int32, panel.shape, 1)
        panel_rows = lax.broadcasted_iota(jnp.int32, panel.shape, 0)
        cols = [
            jnp.broadcast_to(jnp.sum(jnp.where(lanes == base + j, whole, 0.0), 1, keepdims=True), whole.shape)
            for j in range(8)
        ]
        pivots = [
            jnp.broadcast_to(
                jnp.sum(jnp.where(panel_lanes == base + j, panel, 0.0), 1, keepdims=True), panel.shape
            )
            for j in range(8)
        ]
        change = jnp.zeros_like(whole)
        for j in range(8):
            inverse = 1.0 / pivots[j][j : j + 1]
            others = jnp.where(panel_rows != j, pivots[j] * inverse, 0.0)
            scaled = cols[j] * inverse
            for k in range(j + 1, 8):
                head = pivots[k][j : j + 1]
                pivots[k] = pivots[k] - others * head
                cols[k] = cols[k] - scaled * head
            row = panel[j : j + 1]
            change = change + scaled * row
            panel = panel - others * row
        inside = jnp.logical_and(rows >= base, rows < base + 8)
        work_ref[...] = jnp.where(inside, whole, whole - change)
        work_ref[pl.ds(base, 8), :] = panel
        return carry

    lax.fori_loop(0, size // 8, octet, 0)
    done = work_ref[...]
    lanes = lax.broadcasted_iota(jnp.int32, done.shape, 1)
    rows = lax.broadcasted_iota(jnp.int32, done.shape, 0)
    diagonal = jnp.sum(jnp.where(lanes == rows, done, 0.0), 1, keepdims=True)
    return done[:, size:] * (1.0 / diagonal)


def invert(ref, work_ref, between):
    order = ref.shape[0]
    row_ids = lax.broadcasted_iota(jnp.int32, (BLOCK, BLOCK), 0)
    col_ids = lax.broadcasted_iota(jnp.int32, (BLOCK, BLOCK), 1)
    eye = jnp.where(row_ids == col_ids, 1.0, 0.0).astype(jnp.float32)
    for start in range(0, order, BLOCK):
        stop = start + BLOCK
        work_ref[...] = jnp.concatenate([ref[start:stop, start:stop], eye], 1)
        inverse = leaf_inverse(work_ref)
        left = ref[:, start:stop]
        ids = lax.broadcasted_iota(jnp.int32, left.shape, 0)
        left = jnp.where(jnp.logical_and(ids >= start, ids < stop), 0.0, left)
        ref[:, start:stop] = jnp.zeros((order, BLOCK), jnp.float32)
        ref[start:stop, start:stop] = eye
        panel = dot(inverse, ref[start:stop, :])
        ref[start:stop, :] = panel
        ref[...] -= dot(left, panel)
        between(start // BLOCK)


def merge_kernel(
    tiles,
    shared_ref,
    rows_ref,
    own_ref,
    left_ref,
    wide_ref,
    exact_ref,
    z_ref,
    sum_ref,
    part_ref,
    beta_ref,
    pack_ref,
    both_ref,
    far_ref,
    inv_ref,
    couple_ref,
    half_ref,
    other_ref,
    full_ref,
    link_ref,
    temp_ref,
    work_ref,
    middle_ref,
    tall_ref,
    relay_ref,
    z_sems,
    part_sems,
    far_sems,
    line_sems,
    cross_sems,
    twin_sems,
    tall_sems,
    exact_sems,
    relay_sems,
    swap_sems,
    local_sems,
):
    size = shared_ref.shape[-1]
    nodes = shared_ref.shape[1]
    boxes = beta_ref.shape[0]
    slots = tall_ref.shape[0]
    wide_cols, wide_rows = cross_sems.shape[2] + 1, cross_sems.shape[3] + 1
    relays = wide_cols == 2 and wide_rows == 2 and tiles == 2 * boxes
    box_id = lax.axis_index("box")
    tile_id = lax.axis_index("tile")
    core = tile_id % 2
    twin = tile_id + 1 - 2 * core
    own_pair = box_id // 2
    mate = box_id + 1 - 2 * (box_id % 2)
    across = (box_id + 2) % boxes
    chip = tile_id // 2
    row, col = chip // wide_cols, chip % wide_cols

    def tile_at(down, right, on=core):
        return (((row + down + wide_rows) % wide_rows) * wide_cols + (col + right + wide_cols) % wide_cols) * 2 + on

    def remote(source, target, sems, index, box, tile):
        return pltpu.make_async_remote_copy(
            src_ref=source,
            dst_ref=target,
            send_sem=sems.at[(0,) + index],
            recv_sem=sems.at[(1,) + index],
            device_id={"box": box, "tile": tile},
            device_id_type=MESH,
        )

    def each(low, high, action):
        def step(index, carry):
            action(index)
            return carry

        lax.fori_loop(low, high, step, 0)

    barrier = pltpu.get_barrier_semaphore()

    def greet(box, tile):
        pl.semaphore_signal(barrier, inc=1, device_id={"box": box, "tile": tile}, device_id_type=MESH)

    each(1, boxes, lambda i: greet((box_id + i) % boxes, tile_id))
    each(1, tiles, lambda i: greet(box_id, (tile_id + i) % tiles))
    pl.semaphore_wait(barrier, boxes + tiles - 2)

    def chain_step(own, buffer, sems, base, step, sends, action):
        for side, shift in ((0, 1), (1, -1)):
            target = box_id + shift
            origin = box_id - shift * (step - 1) if sends else box_id - shift * step
            valid = jnp.logical_and(origin >= 0, origin < boxes)
            if sends:
                valid = jnp.logical_and(valid, jnp.logical_and(target >= 0, target < boxes))

            @pl.when(valid)
            def _():
                source = own if step == 1 and sends else buffer.at[origin]
                neighbour = (target + boxes) % boxes
                copy = remote(source, buffer.at[origin], sems, (base + side, step - 1), neighbour, tile_id)
                action(copy, origin)

    def start(copy, *rest):
        copy.start()

    def sent(copy, *rest):
        copy.wait_send()

    def came(copy, *rest):
        copy.wait_recv()

    def mate_copy():
        return remote(shared_ref.at[0], z_ref.at[0], z_sems, (0, 0), mate, tile_id)

    def across_copy(pair):
        return remote(sum_ref.at[pair, 0], sum_ref.at[pair, 0], z_sems, (0, 1), across, tile_id)

    def side_copy():
        return remote(shared_ref.at[2], z_ref.at[1], z_sems, (0, 2), across, tile_id)

    def back_copy(side):
        return remote(sum_ref.at[side, 1], sum_ref.at[side, 1], z_sems, (3, 0), mate, tile_id)

    def link_step(step, sends, action):
        chain_step(shared_ref.at[1], beta_ref, z_sems, 1, step, sends, action)

    def part_copy(kind, i, sender):
        tile = (tile_id + i) % tiles
        pair = tile % 2
        if kind == 1:
            source, target = pack_ref.at[pair], both_ref.at[sender]
        else:
            source, target = sum_ref.at[pair, kind // 2], part_ref.at[kind // 2, sender]
        return remote(source, target, part_sems, (kind, i - 1), box_id, tile)

    def part_start(kind, pair):
        def one(i):
            @pl.when((tile_id + i) % 2 == pair)
            def _():
                part_copy(kind, i, tile_id).start()

        each(1, tiles, one)

    def pack(pair):
        pack_ref[pair, :, :size] = beta_ref[2 * pair]
        pack_ref[pair, :, size:] = beta_ref[2 * pair + 1]
        part_start(1, pair)

    mate_copy().start()
    link_step(1, True, start)
    side_copy().start()
    beta_ref[box_id] = shared_ref[1]
    mate_copy().wait_recv()
    sum_ref[own_pair, 0] = shared_ref[0] + z_ref[0]
    across_copy(own_pair).start()
    part_start(0, own_pair)
    link_step(1, False, came)
    link_step(2, True, start)
    pack(own_pair)
    across_copy(1 - own_pair).wait_recv()
    part_start(0, 1 - own_pair)
    side_copy().wait_recv()
    own_side = box_id % 2
    sum_ref[own_side, 1] = shared_ref[2] + z_ref[1]
    back_copy(own_side).start()
    part_start(2, own_side)
    link_step(2, False, came)
    link_step(3, True, start)
    link_step(3, False, came)
    pack(1 - own_pair)
    back_copy(1 - own_side).wait_recv()
    part_start(2, 1 - own_side)
    part_ref[0, tile_id] = sum_ref[core, 0]
    part_ref[1, tile_id] = sum_ref[core, 1]
    both_ref[tile_id] = pack_ref[core]

    def far_step(step, sends, action):
        chain_step(rows_ref, far_ref, far_sems, 0, step, sends, action)

    far_step(1, True, start)

    def line_copy(axis, i, sender):
        dest = tile_at(0, i) if axis == 0 else tile_at(i, 0)
        return remote(rows_ref, wide_ref.at[:, sender], line_sems, (axis, i - 1), box_id, dest)

    def line_source(axis, i):
        return tile_at(0, -i) if axis == 0 else tile_at(-i, 0)

    def cross_copy(axis, i, j, sender):
        dest = tile_at(j, 0) if axis == 0 else tile_at(0, i)
        part = wide_ref.at[pl.ds(2 * axis, 2), sender]
        return remote(part, part, cross_sems, (axis, i - 1, j - 1), box_id, dest)

    def twin_copy(i, j, on):
        sender = tile_at(-j, -i, on)
        source = rows_ref if isinstance(i, int) and isinstance(j, int) else wide_ref.at[:, sender]
        return remote(source, wide_ref.at[:, sender], twin_sems, (i, j), box_id, twin)

    each(1, wide_cols, lambda i: line_copy(0, i, tile_id).start())
    each(1, wide_rows, lambda j: line_copy(1, j, tile_id).start())
    twin_copy(0, 0, core).start()
    keep = pltpu.make_async_copy(rows_ref, wide_ref.at[:, tile_id], local_sems.at[0])
    keep.start()

    def owner(box, face, tile):
        flat = (box * 4 + face) * tiles + tile
        return flat // slots, flat % slots

    def exact_move(face, remote_action, local_action):
        dest, slot = owner(box_id, face, tile_id)
        direct = dest != tile_id

        @pl.when(dest == tile_id)
        def _():
            local_action(
                pltpu.make_async_copy(own_ref.at[face], exact_ref.at[slot], local_sems.at[1 + face])
            )

        if relays:
            dest_row, dest_col = dest // 2 // wide_cols, dest // 2 % wide_cols
            corner = jnp.logical_and(dest_row != row, dest_col != col)
            direct = jnp.logical_and(direct, jnp.logical_not(corner))
            via = tile_at(0, 1) if face % 2 == 0 else tile_at(1, 0)

            @pl.when(corner)
            def _():
                remote_action(
                    pltpu.make_async_remote_copy(
                        src_ref=own_ref.at[face],
                        dst_ref=relay_ref.at[face // 2],
                        send_sem=exact_sems.at[0, face],
                        recv_sem=relay_sems.at[1, face // 2],
                        device_id={"box": box_id, "tile": via},
                        device_id_type=MESH,
                    )
                )

        @pl.when(direct)
        def _():
            remote_action(
                pltpu.make_async_remote_copy(
                    src_ref=own_ref.at[face],
                    dst_ref=exact_ref.at[slot],
                    send_sem=exact_sems.at[0, face],
                    recv_sem=exact_sems.at[1, slot],
                    device_id={"box": box_id, "tile": dest},
                    device_id_type=MESH,
                )
            )

    def relay_move(half, starting):
        dest_chip = owner(box_id, 0, 0)[0] // 2
        dest_row, dest_col = dest_chip // wide_cols, dest_chip % wide_cols

        def one(face, origin):
            dest, slot = owner(box_id, face, origin)
            copy = pltpu.make_async_remote_copy(
                src_ref=relay_ref.at[half],
                dst_ref=exact_ref.at[slot],
                send_sem=relay_sems.at[0, half],
                recv_sem=exact_sems.at[1, slot],
                device_id={"box": box_id, "tile": dest},
                device_id_type=MESH,
            )
            if starting:
                remote(own_ref.at[face], relay_ref.at[half], relay_sems, (half,), box_id, origin).wait_recv()
                copy.start()
            else:
                copy.wait_send()

        @pl.when(jnp.logical_and(col == dest_col, row != dest_row))
        def _():
            one(2 * half, tile_at(0, 1))

        @pl.when(jnp.logical_and(row == dest_row, col != dest_col))
        def _():
            one(2 * half + 1, tile_at(1, 0))

    def tall_move(box, face, starting):
        dest, slot = owner(box, face, tile_id)

        @pl.when(dest == tile_id)
        def _():
            if starting:
                tall_ref[slot] = far_ref[box, face]

        @pl.when(dest != tile_id)
        def _():
            copy = pltpu.make_async_remote_copy(
                src_ref=far_ref.at[box, face],
                dst_ref=tall_ref.at[slot],
                send_sem=tall_sems.at[0, 4 * box + face],
                recv_sem=tall_sems.at[1, slot],
                device_id={"box": box_id, "tile": dest},
                device_id_type=MESH,
            )
            if starting:
                copy.start()
            else:
                copy.wait_send()

    for face in range(4):
        exact_move(face, start, start)

    def spread(step, starting):
        for origin in (box_id - step, box_id + step):

            @pl.when(jnp.logical_and(origin >= 0, origin < boxes))
            def _():
                for face in range(4):
                    tall_move(origin, face, starting)

    def forward_far(step):
        far_step(step, False, came)
        if step < boxes - 1:
            far_step(step + 1, True, start)

        spread(step, True)

    def forward_row(i):
        line_copy(0, i, line_source(0, i)).wait_recv()
        each(1, wide_rows, lambda j: cross_copy(0, i, j, line_source(0, i)).start())
        twin_copy(i, 0, core).start()

    def forward_col(j):
        line_copy(1, j, line_source(1, j)).wait_recv()
        each(1, wide_cols, lambda i: cross_copy(1, i, j, line_source(1, j)).start())
        twin_copy(0 * j, j, core).start()

    def cross_cell(i, j):
        sender = tile_at(-j, -i)
        cross_copy(0, i, j, sender).wait_recv()
        cross_copy(1, i, j, sender).wait_recv()
        twin_copy(i, j, core).start()

    def forward_cross():
        each(1, wide_cols, lambda i: each(1, wide_rows, lambda j: cross_cell(i, j)))

    def forward_line():
        each(1, wide_cols, forward_row)
        each(1, wide_rows, forward_col)

    def forward_relay():
        if relays:
            for half in range(2):
                relay_move(half, True)

    def part_wait(kind):
        each(1, tiles, lambda i: part_copy(kind, i, (tile_id + tiles - i) % tiles).wait_recv())

    def matrix(ref, span):
        if nodes % 8 == 0:
            return ref[...].reshape(tiles * nodes, span)
        for tile in range(tiles):
            middle_ref[tile * nodes : (tile + 1) * nodes, :span] = ref[tile]
        return middle_ref[:size, :span]

    def swap(ref, index):
        return remote(ref, ref, swap_sems, (index,), box_id, twin)

    def half_swap(index):
        return remote(half_ref.at[index], other_ref.at[index], swap_sems, (2 + index,), box_id, twin)

    hooks = {
        (1, 0): lambda: forward_far(1),
        (1, 2): forward_line,
        (1, 5): lambda: forward_far(2),
        (2, 0): forward_cross,
        (2, 2): forward_relay,
        (2, 4): lambda: forward_far(3),
    }

    def stage(index, carry):
        @pl.when(index == 0)
        def _():
            part_wait(0)
            temp_ref[...] = matrix(part_ref.at[0], size)

        @pl.when(index == 1)
        def _():
            inv_ref[core] = temp_ref[...]
            swap(inv_ref.at[core], 0).start()
            part_wait(1)
            linked = matrix(both_ref, 2 * size)
            for side in range(2):
                link_ref[side] = linked[:, side * size : (side + 1) * size]

            def couple(side):
                couple_ref[core, side] = dot(link_ref[side], inv_ref[core])

            each(0, 2, couple)
            swap(couple_ref.at[core], 1).start()
            part_wait(2)
            shared = matrix(part_ref.at[1], size)
            temp_ref[...] = shared

            def term(item):
                side, other = item // 2, (item + 1) // 2
                own = jnp.logical_and(side == other, side == core)
                direct = jnp.where(own, temp_ref[...], 0.0)
                half_ref[item] = direct - dot_nt(couple_ref[core, side], link_ref[other])
                half_swap(item).start()

            each(0, 3, term)
            half_swap(0).wait_recv()
            temp_ref[...] = half_ref[0] + other_ref[0]

        @pl.when(index == 2)
        def _():
            full_ref[0, 0] = temp_ref[...]
            half_swap(1).wait_recv()
            cross = half_ref[1] + other_ref[1]
            link_ref[0] = dot(full_ref[0, 0], cross)
            half_swap(2).wait_recv()
            temp_ref[...] = half_ref[2] + other_ref[2] - dot(cross.T, link_ref[0])

        def between(block):
            for (when, at), action in hooks.items():
                if at == block:
                    pl.when(index == when)(action)

        invert(temp_ref, work_ref, between)
        return carry

    lax.fori_loop(0, 3, stage, 0)
    full_ref[1, 1] = temp_ref[...]
    temp_ref[...] = link_ref[0]
    full_ref[0, 1] = -dot(temp_ref[...], full_ref[1, 1])
    full_ref[1, 0] = full_ref[0, 1].T
    full_ref[0, 0] = full_ref[0, 0] - dot_nt(full_ref[0, 1], temp_ref[...])
    swap(inv_ref.at[1 - core], 0).wait_recv()
    swap(couple_ref.at[1 - core], 1).wait_recv()
    row_box = tile_id * boxes // tiles
    row_pair, row_side = row_box // 2, row_box % 2
    col_pair, col_side = box_id // 2, box_id % 2

    def spread_inverse(item):
        side = jnp.where(item == 2, col_side, item)
        pair = jnp.where(item == 2, row_pair, col_pair)
        link_ref[item] = dot(full_ref[side, 0], couple_ref[pair, 0], HIGH) + dot(
            full_ref[side, 1], couple_ref[pair, 1], HIGH
        )

    each(0, 3, spread_inverse)
    middle_ref[:size, size:] = -link_ref[2].T
    middle_ref[size:, :size] = -link_ref[row_side]
    middle_ref[size:, size:] = full_ref[row_side, col_side]
    corner = dot(couple_ref[row_pair, 0].T, link_ref[0], HIGH) + dot(
        couple_ref[row_pair, 1].T, link_ref[1], HIGH
    )
    middle_ref[:size, :size] = corner + jnp.where(row_pair == col_pair, inv_ref[row_pair], 0.0)

    def twin_wait(i, j):
        twin_copy(i, j, 1 - core).wait_recv()

    each(0, wide_cols, lambda i: each(0, wide_rows, lambda j: twin_wait(i, j)))
    keep.wait()

    def slot_copy(slot):
        flat = tile_id * slots + slot
        source = wide_ref.at[flat // tiles % 4, flat % tiles]
        return pltpu.make_async_copy(source, tall_ref.at[slot], local_sems.at[5 + slot])

    @pl.when(row_box == box_id)
    def _():
        each(0, slots, lambda slot: slot_copy(slot).start())
        each(0, slots, lambda slot: slot_copy(slot).wait())

    def slot_wait(slot):
        source = (tile_id * slots + slot) % tiles

        @pl.when(jnp.logical_and(source != tile_id, row_box != box_id))
        def _():
            remote(rows_ref.at[0], tall_ref.at[slot], tall_sems, (slot,), box_id, twin).wait_recv()

    each(0, slots, slot_wait)
    if nodes % 8 == 0:
        step = slots // 2

        def product(index, carry):
            piece = tall_ref[pl.ds(index * step, step)].reshape(step * nodes, 2 * size)
            rows = pl.ds(pl.multiple_of(index * step * nodes, 8), step * nodes)
            left_ref[rows, :] = dot(piece, middle_ref[...], HIGH)
            return carry

        lax.fori_loop(0, 2, product, 0)
    else:
        for slot in range(slots):
            left_ref[slot * nodes : (slot + 1) * nodes, :] = tall_ref[slot]
        left_ref[...] = dot(left_ref[...], middle_ref[...], HIGH)

    def exact_wait(slot):
        source = (tile_id * slots + slot) % tiles

        @pl.when(jnp.logical_and(source != tile_id, row_box == box_id))
        def _():
            remote(own_ref.at[0], exact_ref.at[slot], exact_sems, (slot,), box_id, twin).wait_recv()

    each(0, slots, exact_wait)

    for face in range(4):
        exact_move(face, sent, lambda copy: copy.wait())
    if relays:
        for half in range(2):
            relay_move(half, False)
    for step in range(1, boxes):
        far_step(step, True, sent)
        link_step(step, True, sent)
        spread(step, False)
    mate_copy().wait_send()
    across_copy(own_pair).wait_send()
    side_copy().wait_send()
    back_copy(own_side).wait_send()
    for kind in range(3):
        each(1, tiles, lambda i: part_copy(kind, i, tile_id).wait_send())
    each(1, wide_cols, lambda i: line_copy(0, i, tile_id).wait_send())
    each(1, wide_rows, lambda j: line_copy(1, j, tile_id).wait_send())

    def cross_sent(i, j):
        cross_copy(0, i, j, line_source(0, i)).wait_send()
        cross_copy(1, i, j, line_source(1, j)).wait_send()

    each(1, wide_cols, lambda i: each(1, wide_rows, lambda j: cross_sent(i, j)))
    each(0, wide_cols, lambda i: each(0, wide_rows, lambda j: twin_copy(i, j, core).wait_send()))
    swap(inv_ref.at[core], 0).wait_send()
    swap(couple_ref.at[core], 1).wait_send()
    for index in range(3):
        half_swap(index).wait_send()


def merge(shared, rows, own):
    _, nodes, size = shared.shape
    tiles, boxes = lax.axis_size("tile"), lax.axis_size("box")
    slots = 4 * boxes
    square = (size, size)
    wide_cols = 1 << ((tiles // 2).bit_length() - 1) // 2
    wide_rows = tiles // 2 // wide_cols

    def vmem(*shape):
        return pltpu.VMEM(shape, jnp.float32)

    def sems(*shape):
        return pltpu.SemaphoreType.DMA((2,) + shape)

    def kernel(*refs):
        merge_kernel(tiles, *refs)

    return pl.pallas_call(
        kernel,
        out_shape=[
            jax.ShapeDtypeStruct((slots * nodes, 2 * size), jnp.float32),
            jax.ShapeDtypeStruct((4, tiles, nodes, 2 * size), jnp.float32),
            jax.ShapeDtypeStruct((slots, nodes, 4 * size), jnp.float32),
        ],
        in_specs=[pl.BlockSpec(memory_space=pltpu.VMEM)] * 3,
        out_specs=[pl.BlockSpec(memory_space=pltpu.VMEM)] + [pl.BlockSpec(memory_space=pltpu.HBM)] * 2,
        scratch_shapes=[
            vmem(2, nodes, size),
            vmem(2, 2, nodes, size),
            vmem(2, tiles, nodes, size),
            vmem(boxes, nodes, size),
            vmem(2, nodes, 2 * size),
            vmem(tiles, nodes, 2 * size),
            vmem(boxes, 4, nodes, 2 * size),
            vmem(2, *square),
            vmem(2, 2, *square),
            vmem(3, *square),
            vmem(3, *square),
            vmem(2, 2, *square),
            vmem(3, *square),
            vmem(*square),
            vmem(BLOCK, 2 * BLOCK),
            vmem(2 * size, 2 * size),
            vmem(slots, nodes, 2 * size),
            vmem(2, nodes, 4 * size),
            sems(4, boxes - 1),
            sems(3, tiles - 1),
            sems(2, boxes - 1),
            sems(2, max(wide_cols, wide_rows)),
            sems(2, wide_cols - 1, wide_rows - 1),
            sems(wide_cols, wide_rows),
            sems(slots),
            sems(slots),
            sems(2),
            sems(5),
            pltpu.SemaphoreType.DMA((5 + slots,)),
        ],
        compiler_params=pltpu.CompilerParams(
            collective_id=0, has_side_effects=True, vmem_limit_bytes=60 * 2**20
        ),
        name="merge",
    )(shared, rows, own)


def per_device(box_maps, face_slots):
    shared, rows, own = pick_faces(box_maps[0], face_slots)
    _, nodes, size = shared.shape
    left, wide, exact = merge(shared, rows, own)
    tiles, boxes = lax.axis_size("tile"), lax.axis_size("box")
    box_id, tile_id = lax.axis_index("box"), lax.axis_index("tile")
    same = tile_id * boxes // tiles == box_id
    exact = jnp.where(same, exact.reshape(left.shape[0], 4 * size), 0.0)
    return exact - dot_nt(left, wide.reshape(4 * tiles * nodes, 2 * size), HIGH)


def solution(mesh):
    return jax.shard_map(
        per_device,
        mesh=mesh,
        in_specs=(P("box", None, "tile", None), P()),
        out_specs=P("tile", "box"),
        check_vma=False,
    )
```

```python
import jax
import jax.numpy as jnp
from jax import lax
from jax.experimental import pallas as pl
from jax.experimental.pallas import tpu as pltpu
from jax.sharding import PartitionSpec as P

MESH = pl.DeviceIdType.MESH
HIGHEST = lax.Precision.HIGHEST
HIGH = lax.Precision.HIGH
BLOCK = 64
LANES = 128


def dot(left, right, precision=HIGHEST):
    return jnp.dot(left, right, precision=precision, preferred_element_type=jnp.float32)


def dot_nt(left, right, precision=HIGHEST):
    return lax.dot_general(
        left, right, (((1,), (1,)), ((), ())), precision=precision, preferred_element_type=jnp.float32
    )


def face_order(box_id):
    along_x, along_y = box_id % 2, box_id // 2
    return 1 - along_x, (along_x, 2 + along_y, 4, 5), 3 - along_y


def pick_kernel(slots_ref, stored_ref, shared_ref, rows_ref, own_ref):
    size = shared_ref.shape[-1]
    box_id = lax.axis_index("box")
    x_face, final_faces, y_face = face_order(box_id)
    slot_of = [slots_ref[box_id, face] for face in (x_face, y_face) + final_faces]
    width = -(-(size + BLOCK) // LANES) * LANES

    def piece(row_slot, col_slot):
        start = col_slot * size
        low = start // LANES * LANES
        window = stored_ref[row_slot, :, pl.ds(pl.multiple_of(low, LANES), width)]
        return jnp.where(start == low, window[:, :size], window[:, BLOCK : BLOCK + size])

    x_slot, y_slot, *finals = slot_of
    shared_ref[0] = piece(x_slot, x_slot)
    shared_ref[1] = piece(y_slot, x_slot)
    shared_ref[2] = piece(y_slot, y_slot)
    for index, row_slot in enumerate(finals):
        rows_ref[index] = jnp.concatenate([piece(row_slot, x_slot), piece(row_slot, y_slot)], 1)
        own_ref[index] = jnp.concatenate([piece(row_slot, col_slot) for col_slot in finals], 1)


def pick_faces(stored, face_slots):
    _, nodes, extent = stored.shape
    size = extent // 6
    return pl.pallas_call(
        pick_kernel,
        out_shape=[
            jax.ShapeDtypeStruct((3, nodes, size), jnp.float32),
            jax.ShapeDtypeStruct((4, nodes, 2 * size), jnp.float32),
            jax.ShapeDtypeStruct((4, nodes, 4 * size), jnp.float32),
        ],
        in_specs=[pl.BlockSpec(memory_space=pltpu.SMEM), pl.BlockSpec(memory_space=pltpu.VMEM)],
        out_specs=[pl.BlockSpec(memory_space=pltpu.VMEM)] * 3,
        name="pick_faces",
    )(face_slots, stored)


def leaf_inverse(work_ref):
    size = work_ref.shape[0]

    def octet(index, carry):
        base = pl.multiple_of(index * 8, 8)
        whole = work_ref[...]
        panel = work_ref[pl.ds(base, 8), :]
        lanes = lax.broadcasted_iota(jnp.int32, whole.shape, 1)
        rows = lax.broadcasted_iota(jnp.int32, whole.shape, 0)
        panel_lanes = lax.broadcasted_iota(jnp.int32, panel.shape, 1)
        panel_rows = lax.broadcasted_iota(jnp.int32, panel.shape, 0)
        cols = [
            jnp.broadcast_to(jnp.sum(jnp.where(lanes == base + j, whole, 0.0), 1, keepdims=True), whole.shape)
            for j in range(8)
        ]
        pivots = [
            jnp.broadcast_to(
                jnp.sum(jnp.where(panel_lanes == base + j, panel, 0.0), 1, keepdims=True), panel.shape
            )
            for j in range(8)
        ]
        change = jnp.zeros_like(whole)
        for j in range(8):
            inverse = 1.0 / pivots[j][j : j + 1]
            others = jnp.where(panel_rows != j, pivots[j] * inverse, 0.0)
            scaled = cols[j] * inverse
            for k in range(j + 1, 8):
                head = pivots[k][j : j + 1]
                pivots[k] = pivots[k] - others * head
                cols[k] = cols[k] - scaled * head
            row = panel[j : j + 1]
            change = change + scaled * row
            panel = panel - others * row
        inside = jnp.logical_and(rows >= base, rows < base + 8)
        work_ref[...] = jnp.where(inside, whole, whole - change)
        work_ref[pl.ds(base, 8), :] = panel
        return carry

    lax.fori_loop(0, size // 8, octet, 0)
    done = work_ref[...]
    lanes = lax.broadcasted_iota(jnp.int32, done.shape, 1)
    rows = lax.broadcasted_iota(jnp.int32, done.shape, 0)
    diagonal = jnp.sum(jnp.where(lanes == rows, done, 0.0), 1, keepdims=True)
    return done[:, size:] * (1.0 / diagonal)


def invert(ref, work_ref, between):
    order = ref.shape[0]
    row_ids = lax.broadcasted_iota(jnp.int32, (BLOCK, BLOCK), 0)
    col_ids = lax.broadcasted_iota(jnp.int32, (BLOCK, BLOCK), 1)
    eye = jnp.where(row_ids == col_ids, 1.0, 0.0).astype(jnp.float32)
    for start in range(0, order, BLOCK):
        stop = start + BLOCK
        work_ref[...] = jnp.concatenate([ref[start:stop, start:stop], eye], 1)
        inverse = leaf_inverse(work_ref)
        left = ref[:, start:stop]
        ids = lax.broadcasted_iota(jnp.int32, left.shape, 0)
        left = jnp.where(jnp.logical_and(ids >= start, ids < stop), 0.0, left)
        ref[:, start:stop] = jnp.zeros((order, BLOCK), jnp.float32)
        ref[start:stop, start:stop] = eye
        panel = dot(inverse, ref[start:stop, :])
        ref[start:stop, :] = panel
        ref[...] -= dot(left, panel)
        between(start // BLOCK)


def merge_kernel(
    tiles,
    shared_ref,
    rows_ref,
    own_ref,
    left_ref,
    wide_ref,
    exact_ref,
    z_ref,
    sum_ref,
    part_ref,
    beta_ref,
    pack_ref,
    both_ref,
    far_ref,
    inv_ref,
    couple_ref,
    half_ref,
    other_ref,
    full_ref,
    link_ref,
    temp_ref,
    work_ref,
    middle_ref,
    tall_ref,
    flip_ref,
    z_sems,
    part_sems,
    far_sems,
    line_sems,
    cross_sems,
    twin_sems,
    tall_sems,
    exact_sems,
    swap_sems,
    pass_sems,
    flip_sems,
    local_sems,
):
    size = shared_ref.shape[-1]
    nodes = shared_ref.shape[1]
    boxes = beta_ref.shape[0]
    slots = tall_ref.shape[0]
    wide_cols, wide_rows = cross_sems.shape[2] + 1, cross_sems.shape[3] + 1
    paired = wide_cols == 2 and wide_rows == 2 and tiles == 2 * boxes
    box_id = lax.axis_index("box")
    tile_id = lax.axis_index("tile")
    core = tile_id % 2
    twin = tile_id + 1 - 2 * core
    own_pair = box_id // 2
    mate = box_id + 1 - 2 * (box_id % 2)
    across = (box_id + 2) % boxes
    chip = tile_id // 2
    row, col = chip // wide_cols, chip % wide_cols

    def tile_at(down, right, on=core):
        return (((row + down + wide_rows) % wide_rows) * wide_cols + (col + right + wide_cols) % wide_cols) * 2 + on

    def remote(source, target, sems, index, box, tile):
        return pltpu.make_async_remote_copy(
            src_ref=source,
            dst_ref=target,
            send_sem=sems.at[(0,) + index],
            recv_sem=sems.at[(1,) + index],
            device_id={"box": box, "tile": tile},
            device_id_type=MESH,
        )

    def each(low, high, action):
        def step(index, carry):
            action(index)
            return carry

        lax.fori_loop(low, high, step, 0)

    barrier = pltpu.get_barrier_semaphore()

    def greet(box, tile):
        pl.semaphore_signal(barrier, inc=1, device_id={"box": box, "tile": tile}, device_id_type=MESH)

    each(1, boxes, lambda i: greet((box_id + i) % boxes, tile_id))
    each(1, tiles, lambda i: greet(box_id, (tile_id + i) % tiles))
    pl.semaphore_wait(barrier, boxes + tiles - 2)

    def chain_step(own, buffer, sems, base, step, sends, action):
        for side, shift in ((0, 1), (1, -1)):
            target = box_id + shift
            origin = box_id - shift * (step - 1) if sends else box_id - shift * step
            valid = jnp.logical_and(origin >= 0, origin < boxes)
            if sends:
                valid = jnp.logical_and(valid, jnp.logical_and(target >= 0, target < boxes))

            @pl.when(valid)
            def _():
                source = own if step == 1 and sends else buffer.at[origin]
                neighbour = (target + boxes) % boxes
                copy = remote(source, buffer.at[origin], sems, (base + side, step - 1), neighbour, tile_id)
                action(copy, origin)

    def start(copy, *rest):
        copy.start()

    def sent(copy, *rest):
        copy.wait_send()

    def came(copy, *rest):
        copy.wait_recv()

    def mate_copy():
        return remote(shared_ref.at[0], z_ref.at[0], z_sems, (0, 0), mate, tile_id)

    def across_copy(pair):
        return remote(sum_ref.at[pair, 0], sum_ref.at[pair, 0], z_sems, (0, 1), across, tile_id)

    def side_copy():
        return remote(shared_ref.at[2], z_ref.at[1], z_sems, (0, 2), across, tile_id)

    def back_copy(side):
        return remote(sum_ref.at[side, 1], sum_ref.at[side, 1], z_sems, (3, 0), mate, tile_id)

    def link_step(step, sends, action):
        chain_step(shared_ref.at[1], beta_ref, z_sems, 1, step, sends, action)

    def part_copy(kind, i, sender):
        tile = (tile_id + i) % tiles
        pair = tile % 2
        if kind == 1:
            source, target = pack_ref.at[pair], both_ref.at[sender]
        else:
            source, target = sum_ref.at[pair, kind // 2], part_ref.at[kind // 2, sender]
        return remote(source, target, part_sems, (kind, i - 1), box_id, tile)

    def part_start(kind, pair):
        def one(i):
            @pl.when(jnp.logical_and((tile_id + i) % 2 == pair, part_direct(kind, i)))
            def _():
                part_copy(kind, i, tile_id).start()

        each(1, tiles, one)

    def part_direct(kind, i):
        if kind == 0 or not paired:
            return tile_id >= 0
        other = (tile_id + i) % tiles // 2
        return jnp.logical_or(other // wide_cols == row, other % wide_cols == col)

    def part_origins():
        return ((tile_at(0, 1, 0), tile_at(1, 0)), (tile_at(1, 0, 1), tile_at(0, 1)))

    def part_relay(kind, starting):
        for way, (origin, dest) in enumerate(part_origins()):
            ref = both_ref.at[origin] if kind == 1 else part_ref.at[1, origin]
            copy = pltpu.make_async_remote_copy(
                src_ref=ref,
                dst_ref=ref,
                send_sem=pass_sems.at[kind - 1, way],
                recv_sem=part_sems.at[1, kind, (dest - origin + tiles) % tiles - 1],
                device_id={"box": box_id, "tile": dest},
                device_id_type=MESH,
            )
            if starting:
                part_copy(kind, (tile_id - origin + tiles) % tiles, origin).wait_recv()
                copy.start()
            else:
                copy.wait_send()

    def pack(pair):
        pack_ref[pair, :, :size] = beta_ref[2 * pair]
        pack_ref[pair, :, size:] = beta_ref[2 * pair + 1]
        part_start(1, pair)

    mate_copy().start()
    link_step(1, True, start)
    side_copy().start()
    beta_ref[box_id] = shared_ref[1]
    mate_copy().wait_recv()
    sum_ref[own_pair, 0] = shared_ref[0] + z_ref[0]
    across_copy(own_pair).start()
    part_start(0, own_pair)
    link_step(1, False, came)
    link_step(2, True, start)
    pack(own_pair)
    across_copy(1 - own_pair).wait_recv()
    part_start(0, 1 - own_pair)
    side_copy().wait_recv()
    own_side = box_id % 2
    sum_ref[own_side, 1] = shared_ref[2] + z_ref[1]
    back_copy(own_side).start()
    part_start(2, own_side)
    link_step(2, False, came)
    link_step(3, True, start)
    link_step(3, False, came)
    pack(1 - own_pair)
    back_copy(1 - own_side).wait_recv()
    part_start(2, 1 - own_side)
    part_ref[0, tile_id] = sum_ref[core, 0]
    part_ref[1, tile_id] = sum_ref[core, 1]
    both_ref[tile_id] = pack_ref[core]

    def far_step(step, sends, action):
        chain_step(rows_ref, far_ref, far_sems, 0, step, sends, action)

    far_step(1, True, start)

    def line_copy(axis, i, sender):
        dest = tile_at(0, i) if axis == 0 else tile_at(i, 0)
        return remote(rows_ref, wide_ref.at[:, sender], line_sems, (axis, i - 1), box_id, dest)

    def line_source(axis, i):
        return tile_at(0, -i) if axis == 0 else tile_at(-i, 0)

    def cross_copy(axis, i, j, sender):
        dest = tile_at(j, 0) if axis == 0 else tile_at(0, i)
        part = wide_ref.at[pl.ds(2 * axis, 2), sender]
        return remote(part, part, cross_sems, (axis, i - 1, j - 1), box_id, dest)

    def twin_copy(i, j, on):
        sender = tile_at(-j, -i, on)
        source = rows_ref if isinstance(i, int) and isinstance(j, int) else wide_ref.at[:, sender]
        return remote(source, wide_ref.at[:, sender], twin_sems, (i, j), box_id, twin)

    keep = pltpu.make_async_copy(rows_ref, wide_ref.at[:, tile_id], local_sems.at[0])
    keep.start()

    def owner(box, face, tile):
        flat = (box * 4 + face) * tiles + tile
        return flat // slots, flat % slots

    def trim(ref, face):
        if paired and face >= 2:
            return ref.at[:, pl.ds(2 * size, 2 * size)]
        return ref

    def exact_copy(source, slot, dest, send_sem, face):
        return pltpu.make_async_remote_copy(
            src_ref=trim(source, face),
            dst_ref=trim(exact_ref.at[slot], face),
            send_sem=send_sem,
            recv_sem=exact_sems.at[1, slot],
            device_id={"box": box_id, "tile": dest},
            device_id_type=MESH,
        )

    def exact_local(face):
        slot = owner(box_id, face, tile_id)[1]
        return pltpu.make_async_copy(
            trim(own_ref.at[face], face), trim(exact_ref.at[slot], face), local_sems.at[1 + face]
        )

    def exact_move(face, remote_action, local_action):
        dest, slot = owner(box_id, face, tile_id)
        @pl.when(dest == tile_id)
        def _():
            local_action(exact_local(face))

        @pl.when(dest != tile_id)
        def _():
            remote_action(exact_copy(own_ref.at[face], slot, dest, exact_sems.at[0, face], face))

    def tall_move(box, face, starting):
        dest, slot = owner(box, face, tile_id)

        @pl.when(dest == tile_id)
        def _():
            if starting:
                tall_ref[slot] = far_ref[box, face]

        @pl.when(dest != tile_id)
        def _():
            copy = pltpu.make_async_remote_copy(
                src_ref=far_ref.at[box, face],
                dst_ref=tall_ref.at[slot],
                send_sem=tall_sems.at[0, 4 * box + face],
                recv_sem=tall_sems.at[1, slot],
                device_id={"box": box_id, "tile": dest},
                device_id_type=MESH,
            )
            if starting:
                copy.start()
            else:
                copy.wait_send()

    def spread(step, starting):
        for origin in (box_id - step, box_id + step):

            @pl.when(jnp.logical_and(origin >= 0, origin < boxes))
            def _():
                for face in range(4):
                    tall_move(origin, face, starting)

    def forward_far(step):
        far_step(step, False, came)
        if step < boxes - 1:
            far_step(step + 1, True, start)

    def forward_row(i):
        line_copy(0, i, line_source(0, i)).wait_recv()
        each(1, wide_rows, lambda j: cross_copy(0, i, j, line_source(0, i)).start())
        twin_copy(i, 0, core).start()

    def forward_col(j):
        line_copy(1, j, line_source(1, j)).wait_recv()
        each(1, wide_cols, lambda i: cross_copy(1, i, j, line_source(1, j)).start())
        twin_copy(0 * j, j, core).start()

    def cross_cell(i, j):
        sender = tile_at(-j, -i)
        cross_copy(0, i, j, sender).wait_recv()
        cross_copy(1, i, j, sender).wait_recv()
        twin_copy(i, j, core).start()

    def forward_cross():
        each(1, wide_cols, lambda i: each(1, wide_rows, lambda j: cross_cell(i, j)))

    def forward_line():
        each(1, wide_cols, forward_row)
        each(1, wide_rows, forward_col)

    def part_wait(kind):
        def one(i):
            origin = (tile_id + tiles - i) % tiles
            fresh = tile_id >= 0
            if kind > 0 and paired:
                for early, _ in part_origins():
                    fresh = jnp.logical_and(fresh, origin != early)

            @pl.when(fresh)
            def _():
                part_copy(kind, i, origin).wait_recv()

        each(1, tiles, one)

    def matrix(ref, span):
        if nodes % 8 == 0:
            return ref[...].reshape(tiles * nodes, span)
        for tile in range(tiles):
            middle_ref[tile * nodes : (tile + 1) * nodes, :span] = ref[tile]
        return middle_ref[:size, :span]

    def swap(ref, index):
        return remote(ref, ref, swap_sems, (index,), box_id, twin)

    def half_swap(index):
        return remote(half_ref.at[index], other_ref.at[index], swap_sems, (2 + index,), box_id, twin)

    def part_forward(kind):
        if paired:
            part_relay(kind, True)

    def line_start():
        part_forward(2)
        each(1, wide_cols, lambda i: line_copy(0, i, tile_id).start())
        each(1, wide_rows, lambda j: line_copy(1, j, tile_id).start())
        twin_copy(0, 0, core).start()

    def exact_start():
        for face in range(4):
            exact_move(face, start, start)

    hooks = {
        (0, 2): lambda: part_forward(1),
        (0, 4): line_start,
        (0, 6): lambda: forward_far(1),
        (1, 0): forward_line,
        (1, 2): lambda: forward_far(2),
        (1, 3): lambda: spread(2, True),
        (1, 4): forward_cross,
        (1, 5): lambda: spread(1, True),
        (1, 6): exact_start,
        (2, 0): lambda: forward_far(3),
        (2, 1): lambda: spread(3, True),
    }

    def stage(index, carry):
        @pl.when(index == 0)
        def _():
            part_wait(0)
            temp_ref[...] = matrix(part_ref.at[0], size)

        @pl.when(index == 1)
        def _():
            inv_ref[core] = temp_ref[...]
            swap(inv_ref.at[core], 0).start()
            part_wait(1)
            linked = matrix(both_ref, 2 * size)
            for side in range(2):
                link_ref[side] = linked[:, side * size : (side + 1) * size]

            def couple(side):
                couple_ref[core, side] = dot(link_ref[side], inv_ref[core])

            each(0, 2, couple)
            swap(couple_ref.at[core], 1).start()
            part_wait(2)
            shared = matrix(part_ref.at[1], size)
            temp_ref[...] = shared

            def term(item):
                side, other = item // 2, (item + 1) // 2
                own = jnp.logical_and(side == other, side == core)
                direct = jnp.where(own, temp_ref[...], 0.0)
                half_ref[item] = direct - dot_nt(couple_ref[core, side], link_ref[other])
                half_swap(item).start()

            each(0, 3, term)
            half_swap(0).wait_recv()
            temp_ref[...] = half_ref[0] + other_ref[0]

        @pl.when(index == 2)
        def _():
            full_ref[0, 0] = temp_ref[...]
            half_swap(1).wait_recv()
            cross = half_ref[1] + other_ref[1]
            link_ref[0] = dot(full_ref[0, 0], cross)
            half_swap(2).wait_recv()
            temp_ref[...] = half_ref[2] + other_ref[2] - dot(cross.T, link_ref[0])

        def between(block):
            for (when, at), action in hooks.items():
                if at == block:
                    pl.when(index == when)(action)

        invert(temp_ref, work_ref, between)
        return carry

    lax.fori_loop(0, 3, stage, 0)
    full_ref[1, 1] = temp_ref[...]
    temp_ref[...] = link_ref[0]
    full_ref[0, 1] = -dot(temp_ref[...], full_ref[1, 1])
    full_ref[1, 0] = full_ref[0, 1].T
    full_ref[0, 0] = full_ref[0, 0] - dot_nt(full_ref[0, 1], temp_ref[...])
    swap(inv_ref.at[1 - core], 0).wait_recv()
    swap(couple_ref.at[1 - core], 1).wait_recv()
    row_box = tile_id * boxes // tiles
    row_pair, row_side = row_box // 2, row_box % 2
    col_pair, col_side = box_id // 2, box_id % 2

    def spread_inverse(item):
        side = jnp.where(item == 2, col_side, item)
        pair = jnp.where(item == 2, row_pair, col_pair)
        link_ref[item] = dot(full_ref[side, 0], couple_ref[pair, 0], HIGH) + dot(
            full_ref[side, 1], couple_ref[pair, 1], HIGH
        )

    each(0, 3, spread_inverse)
    middle_ref[:size, size:] = -link_ref[2].T
    middle_ref[size:, :size] = -link_ref[row_side]
    middle_ref[size:, size:] = full_ref[row_side, col_side]
    corner = dot(couple_ref[row_pair, 0].T, link_ref[0], HIGH) + dot(
        couple_ref[row_pair, 1].T, link_ref[1], HIGH
    )
    middle_ref[:size, :size] = corner + jnp.where(row_pair == col_pair, inv_ref[row_pair], 0.0)

    def twin_wait(i, j):
        twin_copy(i, j, 1 - core).wait_recv()

    each(0, wide_cols, lambda i: each(0, wide_rows, lambda j: twin_wait(i, j)))
    keep.wait()

    def slot_copy(slot):
        flat = tile_id * slots + slot
        source = wide_ref.at[flat // tiles % 4, flat % tiles]
        return pltpu.make_async_copy(source, tall_ref.at[slot], local_sems.at[5 + slot])

    @pl.when(row_box == box_id)
    def _():
        each(0, slots, lambda slot: slot_copy(slot).start())
        each(0, slots, lambda slot: slot_copy(slot).wait())

    def slot_wait(slot):
        source = (tile_id * slots + slot) % tiles

        @pl.when(jnp.logical_and(source != tile_id, row_box != box_id))
        def _():
            remote(rows_ref.at[0], tall_ref.at[slot], tall_sems, (slot,), box_id, twin).wait_recv()

    each(0, slots, slot_wait)
    if nodes % 8 == 0:
        step = slots // 2

        def product(index, carry):
            piece = tall_ref[pl.ds(index * step, step)].reshape(step * nodes, 2 * size)
            rows = pl.ds(pl.multiple_of(index * step * nodes, 8), step * nodes)
            left_ref[rows, :] = dot(piece, middle_ref[...], HIGH)
            return carry

        lax.fori_loop(0, 2, product, 0)
    else:
        for slot in range(slots):
            left_ref[slot * nodes : (slot + 1) * nodes, :] = tall_ref[slot]
        left_ref[...] = dot(left_ref[...], middle_ref[...], HIGH)

    def flip_copy(slot):
        half = exact_ref.at[slot, :, pl.ds(2 * size, 2 * size)]
        return remote(half, flip_ref.at[slot], flip_sems, (slot,), box_id, twin)

    def exact_wait(slot, upper):
        source = (tile_id * slots + slot) % tiles
        face = 0 if upper else 2

        @pl.when(source != tile_id)
        def _():
            exact_copy(own_ref.at[0], slot, twin, exact_sems.at[0, 0], face).wait_recv()
            if upper and paired:
                flip_copy(slot).start()

    for face in range(4):
        exact_move(face, sent, lambda copy: copy.wait())
    if paired:

        @pl.when(jnp.logical_and(row_box == box_id, core == 0))
        def _():
            for slot in (tile_id, tile_id + tiles):
                flip_copy(slot).start()
            each(0, slots, lambda slot: exact_wait(slot, True))
            each(0, slots, lambda slot: flip_copy(slot).wait_send())

        @pl.when(jnp.logical_and(row_box == box_id, core == 1))
        def _():
            each(0, slots, lambda slot: exact_wait(slot, False))
            each(0, slots, lambda slot: flip_copy(slot).wait_recv())
            tall_ref[...] = flip_ref[...].reshape(slots * nodes, 2 * size).T.reshape(slots, nodes, 2 * size)
            mirror = pltpu.make_async_copy(tall_ref, exact_ref.at[:, :, pl.ds(0, 2 * size)], local_sems.at[0])
            mirror.start()
            mirror.wait()

    else:

        @pl.when(row_box == box_id)
        def _():
            each(0, slots, lambda slot: exact_wait(slot, True))

    for step in range(1, boxes):
        far_step(step, True, sent)
        link_step(step, True, sent)
        spread(step, False)
    mate_copy().wait_send()
    across_copy(own_pair).wait_send()
    side_copy().wait_send()
    back_copy(own_side).wait_send()
    def part_sent(kind, i):
        @pl.when(part_direct(kind, i))
        def _():
            part_copy(kind, i, tile_id).wait_send()

    for kind in range(3):
        each(1, tiles, lambda i: part_sent(kind, i))
        if kind > 0 and paired:
            part_relay(kind, False)
    each(1, wide_cols, lambda i: line_copy(0, i, tile_id).wait_send())
    each(1, wide_rows, lambda j: line_copy(1, j, tile_id).wait_send())

    def cross_sent(i, j):
        cross_copy(0, i, j, line_source(0, i)).wait_send()
        cross_copy(1, i, j, line_source(1, j)).wait_send()

    each(1, wide_cols, lambda i: each(1, wide_rows, lambda j: cross_sent(i, j)))
    each(0, wide_cols, lambda i: each(0, wide_rows, lambda j: twin_copy(i, j, core).wait_send()))
    swap(inv_ref.at[core], 0).wait_send()
    swap(couple_ref.at[core], 1).wait_send()
    for index in range(3):
        half_swap(index).wait_send()


def merge(shared, rows, own):
    _, nodes, size = shared.shape
    tiles, boxes = lax.axis_size("tile"), lax.axis_size("box")
    slots = 4 * boxes
    square = (size, size)
    wide_cols = 1 << ((tiles // 2).bit_length() - 1) // 2
    wide_rows = tiles // 2 // wide_cols

    def vmem(*shape):
        return pltpu.VMEM(shape, jnp.float32)

    def sems(*shape):
        return pltpu.SemaphoreType.DMA((2,) + shape)

    def kernel(*refs):
        merge_kernel(tiles, *refs)

    return pl.pallas_call(
        kernel,
        out_shape=[
            jax.ShapeDtypeStruct((slots * nodes, 2 * size), jnp.float32),
            jax.ShapeDtypeStruct((4, tiles, nodes, 2 * size), jnp.float32),
            jax.ShapeDtypeStruct((slots, nodes, 4 * size), jnp.float32),
        ],
        in_specs=[pl.BlockSpec(memory_space=pltpu.VMEM)] * 3,
        out_specs=[pl.BlockSpec(memory_space=pltpu.VMEM)] + [pl.BlockSpec(memory_space=pltpu.HBM)] * 2,
        scratch_shapes=[
            vmem(2, nodes, size),
            vmem(2, 2, nodes, size),
            vmem(2, tiles, nodes, size),
            vmem(boxes, nodes, size),
            vmem(2, nodes, 2 * size),
            vmem(tiles, nodes, 2 * size),
            vmem(boxes, 4, nodes, 2 * size),
            vmem(2, *square),
            vmem(2, 2, *square),
            vmem(3, *square),
            vmem(3, *square),
            vmem(2, 2, *square),
            vmem(3, *square),
            vmem(*square),
            vmem(BLOCK, 2 * BLOCK),
            vmem(2 * size, 2 * size),
            vmem(slots, nodes, 2 * size),
            vmem(slots, nodes, 2 * size),
            sems(4, boxes - 1),
            sems(3, tiles - 1),
            sems(2, boxes - 1),
            sems(2, max(wide_cols, wide_rows)),
            sems(2, wide_cols - 1, wide_rows - 1),
            sems(wide_cols, wide_rows),
            sems(slots),
            sems(slots),
            sems(5),
            pltpu.SemaphoreType.DMA((2, 2)),
            sems(slots),
            pltpu.SemaphoreType.DMA((5 + slots,)),
        ],
        compiler_params=pltpu.CompilerParams(
            collective_id=0, has_side_effects=True, vmem_limit_bytes=60 * 2**20
        ),
        name="merge",
    )(shared, rows, own)


def per_device(box_maps, face_slots):
    shared, rows, own = pick_faces(box_maps[0], face_slots)
    _, nodes, size = shared.shape
    left, wide, exact = merge(shared, rows, own)
    tiles, boxes = lax.axis_size("tile"), lax.axis_size("box")
    box_id, tile_id = lax.axis_index("box"), lax.axis_index("tile")
    same = tile_id * boxes // tiles == box_id
    exact = jnp.where(same, exact.reshape(left.shape[0], 4 * size), 0.0)
    return exact - dot_nt(left, wide.reshape(4 * tiles * nodes, 2 * size), HIGH)


def solution(mesh):
    return jax.shard_map(
        per_device,
        mesh=mesh,
        in_specs=(P("box", None, "tile", None), P()),
        out_specs=P("tile", "box"),
        check_vma=False,
    )
```

```python
import jax
import jax.numpy as jnp
from jax import lax
from jax.experimental import pallas as pl
from jax.experimental.pallas import tpu as pltpu
from jax.sharding import PartitionSpec as P

MESH = pl.DeviceIdType.MESH
HIGHEST = lax.Precision.HIGHEST
HIGH = lax.Precision.HIGH
BLOCK = 64
LANES = 128


def dot(left, right, precision=HIGHEST):
    return jnp.dot(left, right, precision=precision, preferred_element_type=jnp.float32)


def dot_nt(left, right, precision=HIGHEST):
    return lax.dot_general(
        left, right, (((1,), (1,)), ((), ())), precision=precision, preferred_element_type=jnp.float32
    )


def face_order(box_id):
    along_x, along_y = box_id % 2, box_id // 2
    return 1 - along_x, (along_x, 2 + along_y, 4, 5), 3 - along_y


def pick_kernel(slots_ref, stored_ref, shared_ref, rows_ref, own_ref):
    size = shared_ref.shape[-1]
    box_id = lax.axis_index("box")
    x_face, final_faces, y_face = face_order(box_id)
    slot_of = [slots_ref[box_id, face] for face in (x_face, y_face) + final_faces]
    width = -(-(size + BLOCK) // LANES) * LANES

    def piece(row_slot, col_slot):
        start = col_slot * size
        low = start // LANES * LANES
        window = stored_ref[row_slot, :, pl.ds(pl.multiple_of(low, LANES), width)]
        return jnp.where(start == low, window[:, :size], window[:, BLOCK : BLOCK + size])

    x_slot, y_slot, *finals = slot_of
    shared_ref[0] = piece(x_slot, x_slot)
    shared_ref[1] = piece(y_slot, x_slot)
    shared_ref[2] = piece(y_slot, y_slot)
    for index, row_slot in enumerate(finals):
        rows_ref[index] = jnp.concatenate([piece(row_slot, x_slot), piece(row_slot, y_slot)], 1)
        own_ref[index] = jnp.concatenate([piece(row_slot, col_slot) for col_slot in finals], 1)


def pick_faces(stored, face_slots):
    _, nodes, extent = stored.shape
    size = extent // 6
    return pl.pallas_call(
        pick_kernel,
        out_shape=[
            jax.ShapeDtypeStruct((3, nodes, size), jnp.float32),
            jax.ShapeDtypeStruct((4, nodes, 2 * size), jnp.float32),
            jax.ShapeDtypeStruct((4, nodes, 4 * size), jnp.float32),
        ],
        in_specs=[pl.BlockSpec(memory_space=pltpu.SMEM), pl.BlockSpec(memory_space=pltpu.VMEM)],
        out_specs=[pl.BlockSpec(memory_space=pltpu.VMEM)] * 3,
        name="pick_faces",
    )(face_slots, stored)


def leaf_inverse(work_ref):
    size = work_ref.shape[0]

    def octet(index, carry):
        base = pl.multiple_of(index * 8, 8)
        whole = work_ref[...]
        panel = work_ref[pl.ds(base, 8), :]
        lanes = lax.broadcasted_iota(jnp.int32, whole.shape, 1)
        rows = lax.broadcasted_iota(jnp.int32, whole.shape, 0)
        panel_lanes = lax.broadcasted_iota(jnp.int32, panel.shape, 1)
        panel_rows = lax.broadcasted_iota(jnp.int32, panel.shape, 0)
        cols = [
            jnp.broadcast_to(jnp.sum(jnp.where(lanes == base + j, whole, 0.0), 1, keepdims=True), whole.shape)
            for j in range(8)
        ]
        pivots = [
            jnp.broadcast_to(
                jnp.sum(jnp.where(panel_lanes == base + j, panel, 0.0), 1, keepdims=True), panel.shape
            )
            for j in range(8)
        ]
        change = jnp.zeros_like(whole)
        for j in range(8):
            inverse = 1.0 / pivots[j][j : j + 1]
            others = jnp.where(panel_rows != j, pivots[j] * inverse, 0.0)
            scaled = cols[j] * inverse
            for k in range(j + 1, 8):
                head = pivots[k][j : j + 1]
                pivots[k] = pivots[k] - others * head
                cols[k] = cols[k] - scaled * head
            row = panel[j : j + 1]
            change = change + scaled * row
            panel = panel - others * row
        inside = jnp.logical_and(rows >= base, rows < base + 8)
        work_ref[...] = jnp.where(inside, whole, whole - change)
        work_ref[pl.ds(base, 8), :] = panel
        return carry

    lax.fori_loop(0, size // 8, octet, 0)
    done = work_ref[...]
    lanes = lax.broadcasted_iota(jnp.int32, done.shape, 1)
    rows = lax.broadcasted_iota(jnp.int32, done.shape, 0)
    diagonal = jnp.sum(jnp.where(lanes == rows, done, 0.0), 1, keepdims=True)
    return done[:, size:] * (1.0 / diagonal)


def invert(ref, work_ref, between):
    order = ref.shape[0]
    row_ids = lax.broadcasted_iota(jnp.int32, (BLOCK, BLOCK), 0)
    col_ids = lax.broadcasted_iota(jnp.int32, (BLOCK, BLOCK), 1)
    eye = jnp.where(row_ids == col_ids, 1.0, 0.0).astype(jnp.float32)
    for start in range(0, order, BLOCK):
        stop = start + BLOCK
        work_ref[...] = jnp.concatenate([ref[start:stop, start:stop], eye], 1)
        inverse = leaf_inverse(work_ref)
        left = ref[:, start:stop]
        ids = lax.broadcasted_iota(jnp.int32, left.shape, 0)
        left = jnp.where(jnp.logical_and(ids >= start, ids < stop), 0.0, left)
        ref[:, start:stop] = jnp.zeros((order, BLOCK), jnp.float32)
        ref[start:stop, start:stop] = eye
        panel = dot(inverse, ref[start:stop, :])
        ref[start:stop, :] = panel
        ref[...] -= dot(left, panel)
        between(start // BLOCK)


def merge_kernel(
    tiles,
    shared_ref,
    rows_ref,
    own_ref,
    left_ref,
    wide_ref,
    exact_ref,
    z_ref,
    sum_ref,
    part_ref,
    beta_ref,
    pack_ref,
    both_ref,
    far_ref,
    inv_ref,
    couple_ref,
    half_ref,
    other_ref,
    full_ref,
    link_ref,
    temp_ref,
    work_ref,
    middle_ref,
    tall_ref,
    flip_ref,
    z_sems,
    part_sems,
    far_sems,
    line_sems,
    cross_sems,
    twin_sems,
    tall_sems,
    exact_sems,
    swap_sems,
    pass_sems,
    flip_sems,
    local_sems,
):
    size = shared_ref.shape[-1]
    nodes = shared_ref.shape[1]
    boxes = beta_ref.shape[0]
    slots = tall_ref.shape[0]
    wide_cols, wide_rows = cross_sems.shape[2] + 1, cross_sems.shape[3] + 1
    paired = wide_cols == 2 and wide_rows == 2 and tiles == 2 * boxes
    box_id = lax.axis_index("box")
    tile_id = lax.axis_index("tile")
    core = tile_id % 2
    twin = tile_id + 1 - 2 * core
    own_pair = box_id // 2
    mate = box_id + 1 - 2 * (box_id % 2)
    across = (box_id + 2) % boxes
    chip = tile_id // 2
    row, col = chip // wide_cols, chip % wide_cols

    def tile_at(down, right, on=core):
        return (((row + down + wide_rows) % wide_rows) * wide_cols + (col + right + wide_cols) % wide_cols) * 2 + on

    def remote(source, target, sems, index, box, tile):
        return pltpu.make_async_remote_copy(
            src_ref=source,
            dst_ref=target,
            send_sem=sems.at[(0,) + index],
            recv_sem=sems.at[(1,) + index],
            device_id={"box": box, "tile": tile},
            device_id_type=MESH,
        )

    def each(low, high, action):
        def step(index, carry):
            action(index)
            return carry

        lax.fori_loop(low, high, step, 0)

    barrier = pltpu.get_barrier_semaphore()

    def greet(box, tile):
        pl.semaphore_signal(barrier, inc=1, device_id={"box": box, "tile": tile}, device_id_type=MESH)

    each(1, boxes, lambda i: greet((box_id + i) % boxes, tile_id))
    each(1, tiles, lambda i: greet(box_id, (tile_id + i) % tiles))
    pl.semaphore_wait(barrier, boxes + tiles - 2)

    def chain_step(own, buffer, sems, base, step, sends, action):
        for side, shift in ((0, 1), (1, -1)):
            target = box_id + shift
            origin = box_id - shift * (step - 1) if sends else box_id - shift * step
            valid = jnp.logical_and(origin >= 0, origin < boxes)
            if sends:
                valid = jnp.logical_and(valid, jnp.logical_and(target >= 0, target < boxes))

            @pl.when(valid)
            def _():
                source = own if step == 1 and sends else buffer.at[origin]
                neighbour = (target + boxes) % boxes
                copy = remote(source, buffer.at[origin], sems, (base + side, step - 1), neighbour, tile_id)
                action(copy, origin)

    def start(copy, *rest):
        copy.start()

    def sent(copy, *rest):
        copy.wait_send()

    def came(copy, *rest):
        copy.wait_recv()

    def mate_copy():
        return remote(shared_ref.at[0], z_ref.at[0], z_sems, (0, 0), mate, tile_id)

    def across_copy(pair):
        return remote(sum_ref.at[pair, 0], sum_ref.at[pair, 0], z_sems, (0, 1), across, tile_id)

    def side_copy():
        return remote(shared_ref.at[2], z_ref.at[1], z_sems, (0, 2), across, tile_id)

    def back_copy(side):
        return remote(sum_ref.at[side, 1], sum_ref.at[side, 1], z_sems, (3, 0), mate, tile_id)

    def link_step(step, sends, action):
        chain_step(shared_ref.at[1], beta_ref, z_sems, 1, step, sends, action)

    def part_copy(kind, i, sender):
        tile = (tile_id + i) % tiles
        pair = tile % 2
        if kind == 1:
            source, target = pack_ref.at[pair], both_ref.at[sender]
        else:
            source, target = sum_ref.at[pair, kind // 2], part_ref.at[kind // 2, sender]
        return remote(source, target, part_sems, (kind, i - 1), box_id, tile)

    def part_start(kind, pair):
        def one(i):
            @pl.when(jnp.logical_and((tile_id + i) % 2 == pair, part_direct(kind, i)))
            def _():
                part_copy(kind, i, tile_id).start()

        each(1, tiles, one)

    def part_direct(kind, i):
        if kind == 0 or not paired:
            return tile_id >= 0
        other = (tile_id + i) % tiles // 2
        return jnp.logical_or(other // wide_cols == row, other % wide_cols == col)

    def part_origins():
        return ((tile_at(0, 1, 0), tile_at(1, 0)), (tile_at(1, 0, 1), tile_at(0, 1)))

    def part_relay(kind, starting):
        for way, (origin, dest) in enumerate(part_origins()):
            ref = both_ref.at[origin] if kind == 1 else part_ref.at[1, origin]
            copy = pltpu.make_async_remote_copy(
                src_ref=ref,
                dst_ref=ref,
                send_sem=pass_sems.at[kind - 1, way],
                recv_sem=part_sems.at[1, kind, (dest - origin + tiles) % tiles - 1],
                device_id={"box": box_id, "tile": dest},
                device_id_type=MESH,
            )
            if starting:
                part_copy(kind, (tile_id - origin + tiles) % tiles, origin).wait_recv()
                copy.start()
            else:
                copy.wait_send()

    def pack(pair):
        pack_ref[pair, :, :size] = beta_ref[2 * pair]
        pack_ref[pair, :, size:] = beta_ref[2 * pair + 1]
        part_start(1, pair)

    mate_copy().start()
    link_step(1, True, start)
    side_copy().start()
    beta_ref[box_id] = shared_ref[1]
    mate_copy().wait_recv()
    sum_ref[own_pair, 0] = shared_ref[0] + z_ref[0]
    across_copy(own_pair).start()
    part_start(0, own_pair)
    link_step(1, False, came)
    link_step(2, True, start)
    pack(own_pair)
    across_copy(1 - own_pair).wait_recv()
    part_start(0, 1 - own_pair)
    side_copy().wait_recv()
    own_side = box_id % 2
    sum_ref[own_side, 1] = shared_ref[2] + z_ref[1]
    back_copy(own_side).start()
    part_start(2, own_side)
    link_step(2, False, came)
    link_step(3, True, start)
    link_step(3, False, came)
    pack(1 - own_pair)
    back_copy(1 - own_side).wait_recv()
    part_start(2, 1 - own_side)
    part_ref[0, tile_id] = sum_ref[core, 0]
    part_ref[1, tile_id] = sum_ref[core, 1]
    both_ref[tile_id] = pack_ref[core]

    def far_step(step, sends, action):
        chain_step(rows_ref, far_ref, far_sems, 0, step, sends, action)

    far_step(1, True, start)

    def line_copy(axis, i, sender):
        dest = tile_at(0, i) if axis == 0 else tile_at(i, 0)
        return remote(rows_ref, wide_ref.at[:, sender], line_sems, (axis, i - 1), box_id, dest)

    def line_source(axis, i):
        return tile_at(0, -i) if axis == 0 else tile_at(-i, 0)

    def cross_copy(axis, i, j, sender):
        dest = tile_at(j, 0) if axis == 0 else tile_at(0, i)
        part = wide_ref.at[pl.ds(2 * axis, 2), sender]
        return remote(part, part, cross_sems, (axis, i - 1, j - 1), box_id, dest)

    def twin_copy(i, j, on):
        sender = tile_at(-j, -i, on)
        source = rows_ref if isinstance(i, int) and isinstance(j, int) else wide_ref.at[:, sender]
        return remote(source, wide_ref.at[:, sender], twin_sems, (i, j), box_id, twin)

    keep = pltpu.make_async_copy(rows_ref, wide_ref.at[:, tile_id], local_sems.at[0])
    keep.start()

    def owner(box, face, tile):
        flat = (box * 4 + face) * tiles + tile
        return flat // slots, flat % slots

    def trim(ref, face):
        if paired and face >= 2:
            return ref.at[:, pl.ds(2 * size, 2 * size)]
        return ref

    def exact_copy(source, slot, dest, send_sem, face):
        return pltpu.make_async_remote_copy(
            src_ref=trim(source, face),
            dst_ref=trim(exact_ref.at[slot], face),
            send_sem=send_sem,
            recv_sem=exact_sems.at[1, slot],
            device_id={"box": box_id, "tile": dest},
            device_id_type=MESH,
        )

    def exact_local(face):
        slot = owner(box_id, face, tile_id)[1]
        return pltpu.make_async_copy(
            trim(own_ref.at[face], face), trim(exact_ref.at[slot], face), local_sems.at[1 + face]
        )

    def exact_move(face, remote_action, local_action):
        dest, slot = owner(box_id, face, tile_id)
        @pl.when(dest == tile_id)
        def _():
            local_action(exact_local(face))

        @pl.when(dest != tile_id)
        def _():
            remote_action(exact_copy(own_ref.at[face], slot, dest, exact_sems.at[0, face], face))

    def tall_move(box, face, starting):
        dest, slot = owner(box, face, tile_id)

        @pl.when(dest == tile_id)
        def _():
            if starting:
                tall_ref[slot] = far_ref[box, face]

        @pl.when(dest != tile_id)
        def _():
            copy = pltpu.make_async_remote_copy(
                src_ref=far_ref.at[box, face],
                dst_ref=tall_ref.at[slot],
                send_sem=tall_sems.at[0, 4 * box + face],
                recv_sem=tall_sems.at[1, slot],
                device_id={"box": box_id, "tile": dest},
                device_id_type=MESH,
            )
            if starting:
                copy.start()
            else:
                copy.wait_send()

    def spread(step, starting):
        for origin in (box_id - step, box_id + step):

            @pl.when(jnp.logical_and(origin >= 0, origin < boxes))
            def _():
                for face in range(4):
                    tall_move(origin, face, starting)

    def forward_far(step):
        far_step(step, False, came)
        if step < boxes - 1:
            far_step(step + 1, True, start)

    def forward_row(i):
        line_copy(0, i, line_source(0, i)).wait_recv()
        each(1, wide_rows, lambda j: cross_copy(0, i, j, line_source(0, i)).start())
        twin_copy(i, 0, core).start()

    def forward_col(j):
        line_copy(1, j, line_source(1, j)).wait_recv()
        each(1, wide_cols, lambda i: cross_copy(1, i, j, line_source(1, j)).start())
        twin_copy(0 * j, j, core).start()

    def cross_cell(i, j):
        sender = tile_at(-j, -i)
        cross_copy(0, i, j, sender).wait_recv()
        cross_copy(1, i, j, sender).wait_recv()
        twin_copy(i, j, core).start()

    def forward_cross():
        each(1, wide_cols, lambda i: each(1, wide_rows, lambda j: cross_cell(i, j)))

    def forward_line():
        each(1, wide_cols, forward_row)
        each(1, wide_rows, forward_col)

    def part_wait(kind):
        def one(i):
            origin = (tile_id + tiles - i) % tiles
            fresh = tile_id >= 0
            if kind > 0 and paired:
                for early, _ in part_origins():
                    fresh = jnp.logical_and(fresh, origin != early)

            @pl.when(fresh)
            def _():
                part_copy(kind, i, origin).wait_recv()

        each(1, tiles, one)

    def matrix(ref, span):
        if nodes % 8 == 0:
            return ref[...].reshape(tiles * nodes, span)
        for tile in range(tiles):
            middle_ref[tile * nodes : (tile + 1) * nodes, :span] = ref[tile]
        return middle_ref[:size, :span]

    def swap(ref, index):
        return remote(ref, ref, swap_sems, (index,), box_id, twin)

    def half_swap(index):
        return remote(half_ref.at[index], other_ref.at[index], swap_sems, (2 + index,), box_id, twin)

    def part_forward(kind):
        if paired:
            part_relay(kind, True)

    def line_start():
        part_forward(2)
        each(1, wide_cols, lambda i: line_copy(0, i, tile_id).start())
        each(1, wide_rows, lambda j: line_copy(1, j, tile_id).start())
        twin_copy(0, 0, core).start()

    def exact_start():
        for face in range(4):
            exact_move(face, start, start)

    hooks = {
        (0, 2): lambda: part_forward(1),
        (0, 4): line_start,
        (0, 6): lambda: forward_far(1),
        (1, 0): forward_line,
        (1, 2): lambda: forward_far(2),
        (1, 3): forward_cross,
        (1, 4): exact_start,
        (1, 5): lambda: spread(1, True),
        (1, 6): lambda: spread(2, True),
        (2, 0): lambda: forward_far(3),
        (2, 1): lambda: spread(3, True),
    }

    def stage(index, carry):
        @pl.when(index == 0)
        def _():
            part_wait(0)
            temp_ref[...] = matrix(part_ref.at[0], size)

        @pl.when(index == 1)
        def _():
            inv_ref[core] = temp_ref[...]
            swap(inv_ref.at[core], 0).start()
            part_wait(1)
            linked = matrix(both_ref, 2 * size)
            for side in range(2):
                link_ref[side] = linked[:, side * size : (side + 1) * size]

            def couple(side):
                couple_ref[core, side] = dot(link_ref[side], inv_ref[core])

            each(0, 2, couple)
            swap(couple_ref.at[core], 1).start()
            part_wait(2)
            shared = matrix(part_ref.at[1], size)
            temp_ref[...] = shared

            def term(item):
                side, other = item // 2, (item + 1) // 2
                own = jnp.logical_and(side == other, side == core)
                direct = jnp.where(own, temp_ref[...], 0.0)
                half_ref[item] = direct - dot_nt(couple_ref[core, side], link_ref[other])
                half_swap(item).start()

            each(0, 3, term)
            half_swap(0).wait_recv()
            temp_ref[...] = half_ref[0] + other_ref[0]

        @pl.when(index == 2)
        def _():
            full_ref[0, 0] = temp_ref[...]
            half_swap(1).wait_recv()
            cross = half_ref[1] + other_ref[1]
            link_ref[0] = dot(full_ref[0, 0], cross)
            half_swap(2).wait_recv()
            temp_ref[...] = half_ref[2] + other_ref[2] - dot(cross.T, link_ref[0])

        def between(block):
            for (when, at), action in hooks.items():
                if at == block:
                    pl.when(index == when)(action)

        invert(temp_ref, work_ref, between)
        return carry

    lax.fori_loop(0, 3, stage, 0)
    full_ref[1, 1] = temp_ref[...]
    temp_ref[...] = link_ref[0]
    full_ref[0, 1] = -dot(temp_ref[...], full_ref[1, 1])
    full_ref[1, 0] = full_ref[0, 1].T
    full_ref[0, 0] = full_ref[0, 0] - dot_nt(full_ref[0, 1], temp_ref[...])
    swap(inv_ref.at[1 - core], 0).wait_recv()
    swap(couple_ref.at[1 - core], 1).wait_recv()
    row_box = tile_id * boxes // tiles
    row_pair, row_side = row_box // 2, row_box % 2
    col_pair, col_side = box_id // 2, box_id % 2

    def spread_inverse(item):
        side = jnp.where(item == 2, col_side, item)
        pair = jnp.where(item == 2, row_pair, col_pair)
        link_ref[item] = dot(full_ref[side, 0], couple_ref[pair, 0], HIGH) + dot(
            full_ref[side, 1], couple_ref[pair, 1], HIGH
        )

    each(0, 3, spread_inverse)
    middle_ref[:size, size:] = -link_ref[2].T
    middle_ref[size:, :size] = -link_ref[row_side]
    middle_ref[size:, size:] = full_ref[row_side, col_side]
    corner = dot(couple_ref[row_pair, 0].T, link_ref[0], HIGH) + dot(
        couple_ref[row_pair, 1].T, link_ref[1], HIGH
    )
    middle_ref[:size, :size] = corner + jnp.where(row_pair == col_pair, inv_ref[row_pair], 0.0)

    def twin_wait(i, j):
        twin_copy(i, j, 1 - core).wait_recv()

    each(0, wide_cols, lambda i: each(0, wide_rows, lambda j: twin_wait(i, j)))
    keep.wait()

    def slot_copy(slot):
        flat = tile_id * slots + slot
        source = wide_ref.at[flat // tiles % 4, flat % tiles]
        return pltpu.make_async_copy(source, tall_ref.at[slot], local_sems.at[5 + slot])

    @pl.when(row_box == box_id)
    def _():
        each(0, slots, lambda slot: slot_copy(slot).start())
        each(0, slots, lambda slot: slot_copy(slot).wait())

    def slot_wait(slot):
        source = (tile_id * slots + slot) % tiles

        @pl.when(jnp.logical_and(source != tile_id, row_box != box_id))
        def _():
            remote(rows_ref.at[0], tall_ref.at[slot], tall_sems, (slot,), box_id, twin).wait_recv()

    each(0, slots, slot_wait)
    if nodes % 8 == 0:
        step = slots // 2

        def product(index, carry):
            piece = tall_ref[pl.ds(index * step, step)].reshape(step * nodes, 2 * size)
            rows = pl.ds(pl.multiple_of(index * step * nodes, 8), step * nodes)
            left_ref[rows, :] = dot(piece, middle_ref[...], HIGH)
            return carry

        lax.fori_loop(0, 2, product, 0)
    else:
        for slot in range(slots):
            left_ref[slot * nodes : (slot + 1) * nodes, :] = tall_ref[slot]
        left_ref[...] = dot(left_ref[...], middle_ref[...], HIGH)

    def flip_copy(slot):
        half = exact_ref.at[slot, :, pl.ds(2 * size, 2 * size)]
        return remote(half, flip_ref.at[slot], flip_sems, (slot,), box_id, twin)

    def exact_wait(slot, upper):
        source = (tile_id * slots + slot) % tiles
        face = 0 if upper else 2

        @pl.when(source != tile_id)
        def _():
            exact_copy(own_ref.at[0], slot, twin, exact_sems.at[0, 0], face).wait_recv()
            if upper and paired:
                flip_copy(slot).start()

    for face in range(4):
        exact_move(face, sent, lambda copy: copy.wait())
    if paired:

        @pl.when(jnp.logical_and(row_box == box_id, core == 0))
        def _():
            for slot in (tile_id, tile_id + tiles):
                flip_copy(slot).start()
            each(0, slots, lambda slot: exact_wait(slot, True))
            each(0, slots, lambda slot: flip_copy(slot).wait_send())

        @pl.when(jnp.logical_and(row_box == box_id, core == 1))
        def _():
            each(0, slots, lambda slot: exact_wait(slot, False))
            each(0, slots, lambda slot: flip_copy(slot).wait_recv())
            tall_ref[...] = flip_ref[...].reshape(slots * nodes, 2 * size).T.reshape(slots, nodes, 2 * size)
            mirror = pltpu.make_async_copy(tall_ref, exact_ref.at[:, :, pl.ds(0, 2 * size)], local_sems.at[0])
            mirror.start()
            mirror.wait()

    else:

        @pl.when(row_box == box_id)
        def _():
            each(0, slots, lambda slot: exact_wait(slot, True))

    for step in range(1, boxes):
        far_step(step, True, sent)
        link_step(step, True, sent)
        spread(step, False)
    mate_copy().wait_send()
    across_copy(own_pair).wait_send()
    side_copy().wait_send()
    back_copy(own_side).wait_send()
    def part_sent(kind, i):
        @pl.when(part_direct(kind, i))
        def _():
            part_copy(kind, i, tile_id).wait_send()

    for kind in range(3):
        each(1, tiles, lambda i: part_sent(kind, i))
        if kind > 0 and paired:
            part_relay(kind, False)
    each(1, wide_cols, lambda i: line_copy(0, i, tile_id).wait_send())
    each(1, wide_rows, lambda j: line_copy(1, j, tile_id).wait_send())

    def cross_sent(i, j):
        cross_copy(0, i, j, line_source(0, i)).wait_send()
        cross_copy(1, i, j, line_source(1, j)).wait_send()

    each(1, wide_cols, lambda i: each(1, wide_rows, lambda j: cross_sent(i, j)))
    each(0, wide_cols, lambda i: each(0, wide_rows, lambda j: twin_copy(i, j, core).wait_send()))
    swap(inv_ref.at[core], 0).wait_send()
    swap(couple_ref.at[core], 1).wait_send()
    for index in range(3):
        half_swap(index).wait_send()


def merge(shared, rows, own):
    _, nodes, size = shared.shape
    tiles, boxes = lax.axis_size("tile"), lax.axis_size("box")
    slots = 4 * boxes
    square = (size, size)
    wide_cols = 1 << ((tiles // 2).bit_length() - 1) // 2
    wide_rows = tiles // 2 // wide_cols

    def vmem(*shape):
        return pltpu.VMEM(shape, jnp.float32)

    def sems(*shape):
        return pltpu.SemaphoreType.DMA((2,) + shape)

    def kernel(*refs):
        merge_kernel(tiles, *refs)

    return pl.pallas_call(
        kernel,
        out_shape=[
            jax.ShapeDtypeStruct((slots * nodes, 2 * size), jnp.float32),
            jax.ShapeDtypeStruct((4, tiles, nodes, 2 * size), jnp.float32),
            jax.ShapeDtypeStruct((slots, nodes, 4 * size), jnp.float32),
        ],
        in_specs=[pl.BlockSpec(memory_space=pltpu.VMEM)] * 3,
        out_specs=[pl.BlockSpec(memory_space=pltpu.VMEM)] + [pl.BlockSpec(memory_space=pltpu.HBM)] * 2,
        scratch_shapes=[
            vmem(2, nodes, size),
            vmem(2, 2, nodes, size),
            vmem(2, tiles, nodes, size),
            vmem(boxes, nodes, size),
            vmem(2, nodes, 2 * size),
            vmem(tiles, nodes, 2 * size),
            vmem(boxes, 4, nodes, 2 * size),
            vmem(2, *square),
            vmem(2, 2, *square),
            vmem(3, *square),
            vmem(3, *square),
            vmem(2, 2, *square),
            vmem(3, *square),
            vmem(*square),
            vmem(BLOCK, 2 * BLOCK),
            vmem(2 * size, 2 * size),
            vmem(slots, nodes, 2 * size),
            vmem(slots, nodes, 2 * size),
            sems(4, boxes - 1),
            sems(3, tiles - 1),
            sems(2, boxes - 1),
            sems(2, max(wide_cols, wide_rows)),
            sems(2, wide_cols - 1, wide_rows - 1),
            sems(wide_cols, wide_rows),
            sems(slots),
            sems(slots),
            sems(5),
            pltpu.SemaphoreType.DMA((2, 2)),
            sems(slots),
            pltpu.SemaphoreType.DMA((5 + slots,)),
        ],
        compiler_params=pltpu.CompilerParams(
            collective_id=0, has_side_effects=True, vmem_limit_bytes=60 * 2**20
        ),
        name="merge",
    )(shared, rows, own)


def per_device(box_maps, face_slots):
    shared, rows, own = pick_faces(box_maps[0], face_slots)
    _, nodes, size = shared.shape
    left, wide, exact = merge(shared, rows, own)
    tiles, boxes = lax.axis_size("tile"), lax.axis_size("box")
    box_id, tile_id = lax.axis_index("box"), lax.axis_index("tile")
    same = tile_id * boxes // tiles == box_id
    exact = exact.reshape(left.shape[0], 4 * size)
    change = dot_nt(left, wide.reshape(4 * tiles * nodes, 2 * size), HIGH)
    return jnp.where(same, exact - change, -change)


def solution(mesh):
    return jax.shard_map(
        per_device,
        mesh=mesh,
        in_specs=(P("box", None, "tile", None), P()),
        out_specs=P("tile", "box"),
        check_vma=False,
    )
```
